32 devices in a mesh: row: 8 (over z, y), col: 4 (over x, core).
Axes of the slice: x: 2, y: 2, z: 4, core: 2. Of those that a mesh axis runs over, the one named last changes fastest.
Arguments:
- grams: bfloat16 [4, 3584, 3584], P(None, 'row', 'col'), as said below
- weights: bfloat16 [4, 3584, 7168], P(None, 'row', 'col'), may hold values from -6 to 6
Outputs:
- merged: float32 [3584, 7168], P('row', 'col')
- residual: float32 [3584, 7168], P('row', 'col')
The draws below stay inside these ranges and needn't reach their ends.
Inputs may be any that keep to these rules, and one draw needn't show every extreme that they name: `grams`: each of the 4 matrices is symmetric and positive definite.
All inputs are finite; a program needn't handle non-finite values.
Results may differ from the reference program's by a relative error of at most 0.012.
The reference program's roundings to bfloat16 on the way (of `rounded`) count: a program that leaves them out, or rounds other values in their place, can miss the bound.
Values may be sent and summed in bfloat16 or wider, within the bound.
A program may use at most 256 MiB of HBM per device.

```python
import math
import jax
import jax.numpy as jnp
from jax import lax

D = 3584
FF_COLS = 7168
MODELS = 4
ITERS = 2


def draw_grams(key, part):

    def one_model(model_key):
        scale_key, noise_key = jax.random.split(model_key)
        lowest, highest, spread = (0.5, 5.0, 0.3)
        scales = jnp.exp(jax.random.uniform(scale_key, (D,), jnp.float32, math.log(lowest), math.log(highest)))
        roots = jnp.sqrt(scales)
        noise = jax.random.normal(noise_key, (D, D), jnp.float32) * (spread / math.sqrt(D))
        core = jnp.eye(D, dtype=jnp.float32) + (noise + noise.T) * 0.5
        return (core * (roots[:, None] * roots[None, :])).astype(jnp.bfloat16)
    model_keys = jax.random.split(jax.random.fold_in(key, 17), MODELS)
    return jax.vmap(one_model)(model_keys)


def shard_levels(stream_key, shape, cuts, smallest, high):
    def one(position, parts):
        draws = jax.random.uniform(jax.random.fold_in(jax.random.fold_in(stream_key, 6), position), (parts,), jnp.float32, smallest / len(cuts), high / len(cuts))
        return jnp.repeat(jnp.exp(draws), shape[position] // parts).reshape((-1,) + (1,) * (len(shape) - position - 1))

    factor_of = one(*cuts[0])
    for cut in cuts[1:]:
        factor_of = factor_of * one(*cut)
    return factor_of


def bell_draw(rng, shape, width, limit, pieces=(), kind=jnp.bfloat16):
    factor_of = shard_levels(rng, shape, pieces, -0.22, 0.18) if pieces else 1.0
    values = jax.random.normal(rng, shape, jnp.float32) * width * factor_of
    return jnp.minimum(jnp.maximum(values, -limit), limit).astype(kind)


def setup_inputs(seed: int = 0) -> dict:
    streams_of = jax.random.split(jax.random.key(seed), 3)
    return {
        "grams": draw_grams(jax.random.fold_in(streams_of[2], 71), 0),
        "weights": bell_draw(streams_of[1], (MODELS, D, FF_COLS), 1.0, 6.0, ((1, 8), (2, 4))),
    }


def reference(grams, weights):
    high = lax.Precision.HIGHEST
    total = jnp.zeros((D, D), jnp.float32)
    right_side = jnp.zeros((D, FF_COLS), jnp.float32)
    for model_index in range(MODELS):
        gram_full = grams[model_index].astype(jnp.float32)
        weight = weights[model_index].astype(jnp.float32)
        gram_diag = jnp.diagonal(gram_full)
        right_side = right_side + 0.9 * jnp.dot(gram_full, weight, precision=high) + 0.1 * gram_diag[:, None] * weight
        total = total + gram_full
    total_diag = jnp.diagonal(total)
    merged = jnp.zeros((D, FF_COLS), jnp.float32)
    residual = right_side
    direction = right_side
    norm_now = jnp.sum(residual * residual, axis=0)
    for iteration in range(ITERS):
        rounded = lax.optimization_barrier(direction.astype(jnp.bfloat16)).astype(jnp.float32)
        mapped = 0.9 * jnp.dot(total, rounded, precision=high) + 0.1 * total_diag[:, None] * rounded
        curvature = jnp.sum(direction * mapped, axis=0)
        step_length = norm_now / curvature
        merged = merged + step_length * direction
        residual = residual - step_length * mapped
        if iteration + 1 < ITERS:
            norm_next = jnp.sum(residual * residual, axis=0)
            direction = residual + (norm_next / norm_now) * direction
            norm_now = norm_next
    return merged, residual
```

```python
import functools

import jax
import jax.numpy as jnp
from jax import lax
from jax.experimental import pallas as pl
from jax.experimental.pallas import tpu as pltpu
from jax.sharding import PartitionSpec as P

ITERS = 2
STREAMS = 2
MESH = pl.DeviceIdType.MESH
VMEM_BYTES = 63 * 2**20


def ring_position(index, n):
    odd = index % 2
    return (1 - odd) * (index // 2) + odd * (n - 1 - index // 2)


def ring_index(position, n):
    back = position // (n // 2)
    return (1 - back) * 2 * position + back * (2 * (n - 1 - position) + 1)


def remote(source, target, send, recv, where):
    return pltpu.make_async_remote_copy(
        src_ref=source, dst_ref=target, send_sem=send, recv_sem=recv, device_id=where, device_id_type=MESH
    )


def row_gather_kernel(n, x_ref, d_ref, out_ref, dout_ref, send_a, recv_a, send_b, recv_b):
    me = lax.axis_index("row")
    place = ring_position(me, n)
    right = {"row": ring_index((place + 1) % n, n)}
    left = {"row": ring_index((place + n - 1) % n, n)}
    rows = x_ref.shape[0]
    cut = rows // 32 * 16
    hops = n // 2

    barrier = pltpu.get_barrier_semaphore()
    for other in (left, right):
        pl.semaphore_signal(barrier, inc=1, device_id=other, device_id_type=MESH)
    pl.semaphore_wait(barrier, 2)

    def pair(hop, window):
        ahead = ring_index((place + n - hop) % n, n)
        behind = ring_index((place + hop) % n, n)
        first, second = window
        out = []
        for slot, (held, wa, wb) in enumerate(((out_ref, first, second), (dout_ref, None, None))):
            a = held.at[ahead] if wa is None else held.at[ahead, wa, :]
            b = held.at[behind] if wb is None else held.at[behind, wb, :]
            out.append(remote(a, a, send_a.at[slot, hop], recv_a.at[slot, hop], right))
            out.append(remote(b, b, send_b.at[slot, hop], recv_b.at[slot, hop], left))
        return out

    out_ref[me] = x_ref[...]
    dout_ref[me] = d_ref[...]
    whole = (pl.ds(0, rows), pl.ds(0, rows))
    last = (pl.ds(0, cut), pl.ds(cut, rows - cut))
    for hop in range(hops):
        copies = pair(hop, last if hop == hops - 1 else whole)
        if hop == hops - 1:
            copies = copies[:3]
        for copy in copies:
            copy.start()
        for copy in copies:
            copy.wait()


def row_gather(n, slab, diag):
    shape = jax.ShapeDtypeStruct((n,) + slab.shape, slab.dtype)
    dshape = jax.ShapeDtypeStruct((n,) + diag.shape, diag.dtype)
    vmem = pl.BlockSpec(memory_space=pltpu.VMEM)
    return pl.pallas_call(
        functools.partial(row_gather_kernel, n),
        out_shape=(shape, dshape),
        in_specs=[vmem] * 2,
        out_specs=(vmem, vmem),
        scratch_shapes=[pltpu.SemaphoreType.DMA((2, n // 2))] * 4,
        compiler_params=pltpu.CompilerParams(collective_id=1, has_side_effects=True, vmem_limit_bytes=VMEM_BYTES),
        cost_estimate=pl.CostEstimate(flops=0, bytes_accessed=200 * 2**20, transcendentals=0),
    )(slab, diag)


def col_gather_kernel(parts, pieces, x_ref, d_ref, out_ref, dout_ref, own, copied, send, recv, dsend, drecv):
    me = lax.axis_index("col")
    chips = parts // 2
    chip, core = me // 2, me % 2
    twin = {"col": chip * 2 + 1 - core}
    rows = x_ref.shape[0] // pieces
    barrier = pltpu.get_barrier_semaphore()
    for k in range(1, parts):
        pl.semaphore_signal(barrier, inc=1, device_id={"col": (me + k) % parts}, device_id_type=MESH)
    pl.semaphore_wait(barrier, parts - 1)

    def peer(k):
        return {"col": (chip + k) % chips * 2 + core}

    def window(piece):
        return pl.ds(piece * rows, rows)

    started = []
    for piece in range(pieces):
        for k in list(range(1, chips)) + [0]:
            copy = remote(
                x_ref.at[window(piece), :],
                out_ref.at[me, window(piece), :],
                send.at[k, piece],
                recv.at[k, piece],
                peer(k) if k else twin,
            )
            copy.start()
            started.append(copy)
    dcopies = []
    dout_ref[me] = d_ref[...]
    for k in range(1, parts):
        copy = remote(d_ref, dout_ref.at[me], dsend.at[k], drecv.at[k], {"col": (me + k) % parts})
        copy.start()
        dcopies.append(copy)
    mine = pltpu.make_async_copy(x_ref, out_ref.at[me], own)
    mine.start()
    forwards = []
    for piece in range(pieces):
        for k in range(1, chips):
            origin = (chip + chips - k) % chips * 2 + core
            part = out_ref.at[origin, window(piece), :]
            remote(part, part, send.at[k, piece], recv.at[k, piece], twin).wait_recv()
            copy = remote(part, part, send.at[chips + k - 1, piece], recv.at[chips + k - 1, piece], twin)
            copy.start()
            forwards.append(copy)
    for piece in range(pieces):
        for k in range(chips):
            copy = started[piece * chips + (k - 1) % chips]
            copy.wait_send()
            if k == 0:
                copy.wait_recv()
    for copy in forwards + dcopies:
        copy.wait()
    mine.wait()


def col_gather(parts, slabs, diags):
    pieces = 4
    any_space = pl.BlockSpec(memory_space=pl.ANY)
    vmem = pl.BlockSpec(memory_space=pltpu.VMEM)
    sems = pltpu.SemaphoreType.DMA((parts, pieces))
    return pl.pallas_call(
        functools.partial(col_gather_kernel, parts, pieces),
        out_shape=(
            jax.ShapeDtypeStruct((parts,) + slabs.shape, slabs.dtype),
            jax.ShapeDtypeStruct((parts,) + diags.shape, diags.dtype),
        ),
        in_specs=[vmem] * 2,
        out_specs=(any_space, vmem),
        scratch_shapes=[
            pltpu.SemaphoreType.DMA,
            pltpu.SemaphoreType.DMA,
            sems,
            sems,
            pltpu.SemaphoreType.DMA((parts,)),
            pltpu.SemaphoreType.DMA((parts,)),
        ],
        compiler_params=pltpu.CompilerParams(collective_id=2, has_side_effects=True, vmem_limit_bytes=24 * 2**20),
        cost_estimate=pl.CostEstimate(flops=0, bytes_accessed=400 * 2**20, transcendentals=0),
    )(slabs, diags)


def solve_kernel(
    n, parts, hi_ref, lo_ref, t_ref, d_ref, om_ref, or_ref,
    tv, v, lo, direction, residual, mapped, out_m, out_r, t_sem, send, recv,
):
    me = lax.axis_index("row")
    rows, q = hi_ref.shape[1], hi_ref.shape[2]
    depth = tv.shape[2]
    f32 = jnp.float32

    barrier = pltpu.get_barrier_semaphore()
    for k in range(1, n):
        pl.semaphore_signal(barrier, inc=1, device_id={"row": (me + k) % n}, device_id_type=MESH)
    loads = [pltpu.make_async_copy(t_ref.at[c], tv.at[c], t_sem.at[c]) for c in range(parts)]
    for load in loads:
        load.start()
    pl.semaphore_wait(barrier, n - 1)

    def block(i):
        return pl.ds(pl.multiple_of(i * rows, 16), rows)

    def moved(kind, k, source, target):
        other = (me + k) % n
        return remote(source(other), target, send.at[kind, k], recv.at[kind, k], {"row": other})

    incoming = [
        [moved(0, k, lambda i: hi_ref.at[i], v.at[block(me), :]) for k in range(1, n)],
        [moved(1, k, lambda i: lo_ref.at[i], lo.at[block(me), :]) for k in range(1, n)],
    ]
    for group in incoming:
        for copy in group:
            copy.start()
    v[block(me), :] = hi_ref[me]
    lo[block(me), :] = lo_ref[me]

    def product(_):
        def step(i, carry):
            here = block(i)
            total = jnp.zeros((rows, q), f32)
            for c in range(parts):
                total += jnp.dot(tv[c, here, :], v[pl.ds(c * depth, depth), :], preferred_element_type=f32)
            mapped[here, :] = 0.9 * total + d_ref[here, :] * v[here, :].astype(f32)
            return carry

        lax.fori_loop(0, n, step, 0)

    def column_sum(terms):
        def step(i, total):
            return total + jnp.sum(terms(block(i)), axis=0, keepdims=True)

        return lax.fori_loop(0, n, step, jnp.zeros((1, q), f32))

    for copy in incoming[0]:
        copy.wait()
    for load in loads:
        load.wait()
    product(0)
    for copy in incoming[1]:
        copy.wait()

    def first(here):
        start = v[here, :].astype(f32) + lo[here, :].astype(f32)
        direction[here, :] = start
        return start * start

    norm = column_sum(first)
    curvature = column_sum(lambda here: direction[here, :] * mapped[here, :])
    step_a = norm / curvature

    def second(here):
        left = direction[here, :] - step_a * mapped[here, :]
        residual[here, :] = left
        return left * left

    norm_next = column_sum(second)
    scale = norm_next / norm

    def turn(i, carry):
        here = block(i)
        v[here, :] = (residual[here, :] + scale * direction[here, :]).astype(jnp.bfloat16)
        return carry

    lax.fori_loop(0, n, turn, 0)
    product(0)
    curvature = column_sum(lambda here: (residual[here, :] + scale * direction[here, :]) * mapped[here, :])
    step_b = norm_next / curvature

    def leaving(k):
        i = (me + k) % n
        return [
            remote(held.at[block(i), :], target.at[me], send.at[kind, k], recv.at[kind, k], {"row": i})
            for kind, held, target in ((2, out_m, om_ref), (3, out_r, or_ref))
        ]

    def outputs(i):
        here = block(i)
        left, start = residual[here, :], direction[here, :]
        merged = step_a * start + step_b * (left + scale * start)
        return merged.astype(jnp.bfloat16), (left - step_b * mapped[here, :]).astype(jnp.bfloat16)

    def finish(k, carry):
        i = (me + k) % n
        here = block(i)
        out_m[here, :], out_r[here, :] = outputs(i)

        @pl.when(k > 1)
        def _():
            for copy in leaving(k - 1):
                copy.start()

        return carry

    lax.fori_loop(1, n, finish, 0)
    om_ref[me], or_ref[me] = outputs(me)
    for copy in leaving(n - 1):
        copy.start()

    def drain(k, carry):
        for copy in leaving(k):
            copy.wait()
        return carry

    lax.fori_loop(1, n, drain, 0)


def solve(n, high, low, total, diag):
    parts = total.shape[0]
    _, rows, q = high.shape
    vmem = pl.BlockSpec(memory_space=pltpu.VMEM)
    half, full = pltpu.VMEM((n * rows, q), jnp.bfloat16), pltpu.VMEM((n * rows, q), jnp.float32)
    out = jax.ShapeDtypeStruct((n, rows, q), jnp.bfloat16)
    return pl.pallas_call(
        functools.partial(solve_kernel, n, parts),
        out_shape=(out, out),
        in_specs=[vmem, vmem, pl.BlockSpec(memory_space=pl.ANY), vmem],
        out_specs=(vmem, vmem),
        scratch_shapes=[
            pltpu.VMEM(total.shape, jnp.bfloat16),
            half,
            half,
            full,
            full,
            full,
            half,
            half,
            pltpu.SemaphoreType.DMA((parts,)),
            pltpu.SemaphoreType.DMA((4, n)),
            pltpu.SemaphoreType.DMA((4, n)),
        ],
        compiler_params=pltpu.CompilerParams(collective_id=3, has_side_effects=True, vmem_limit_bytes=VMEM_BYTES),
    )(high, low, total, diag)


def shards(row_count, col_parts, grams, weights):
    models, slab_rows, slab_cols = grams.shape
    col_count = weights.shape[2]
    row_index = lax.axis_index("row")
    width = col_count // STREAMS

    own_total = jnp.sum(grams.astype(jnp.float32), axis=0)
    row_ids = row_index * slab_rows + jnp.arange(slab_rows)[:, None]
    col_ids = lax.axis_index("col") * slab_cols + jnp.arange(slab_cols)[None, :]
    diagonal = row_ids == col_ids
    slab = jnp.where(diagonal, 0.0, own_total).astype(jnp.bfloat16)
    own_diag = jnp.sum(jnp.where(diagonal, own_total, 0.0), axis=1)
    padded = -(-slab_rows // 1024) * 1024
    own_diag = jnp.pad(own_diag, (0, padded - slab_rows)).reshape(-1, 128)
    slabs, some_diags = row_gather(row_count, slab, own_diag)

    gathered = lax.all_gather(grams, "col", axis=0)
    parts = gathered.shape[0]

    def own_columns(array):
        per_slab = slab_cols // slab_rows
        piece = lax.dynamic_index_in_dim(array, row_index // per_slab, 0, keepdims=False)
        offset = (row_index % per_slab) * slab_rows
        return lax.dynamic_slice_in_dim(piece, offset, slab_rows, piece.ndim - 1)

    block = own_columns(gathered)
    on_diag = jnp.arange(slab_rows)[:, None] == jnp.arange(slab_rows)[None, :]
    diags = jnp.sum(jnp.where(on_diag, block.astype(jnp.float32), 0.0), axis=2)
    first_part = (((0,), (0,)), ((), ()))
    depth = models * slab_rows
    flat = gathered.reshape(parts, depth, slab_cols)
    flat_block = block.reshape(depth, slab_rows)
    in_block = (jnp.arange(parts * slab_cols) // slab_rows) == row_index

    def right_side(weight):
        flat_weight = weight.reshape(depth, width)
        pieces = []
        for d in range(parts):
            piece = lax.dot_general(flat[d], flat_weight, first_part, preferred_element_type=jnp.float32)
            keep = in_block[d * slab_cols : (d + 1) * slab_cols]
            pieces.append(jnp.where(keep[:, None], 0.0, piece).astype(jnp.bfloat16))
        others = lax.psum_scatter(jnp.concatenate(pieces, axis=0), "row", scatter_dimension=0, tiled=True)
        own = lax.dot_general(flat_block, flat_weight, first_part, preferred_element_type=jnp.float32)
        diag_term = jnp.sum(diags[:, :, None] * weight.astype(jnp.float32), axis=0)
        return 0.9 * (own + others.astype(jnp.float32)) + 0.1 * diag_term

    starts = [right_side(lax.slice_in_dim(weights, s * width, (s + 1) * width, axis=2)) for s in range(STREAMS)]
    start = jnp.concatenate(starts, axis=1)

    total, diag_slabs = col_gather(col_parts, slabs.reshape(-1, slab_cols), some_diags)
    diag = jnp.sum(diag_slabs.reshape(col_parts, row_count, padded), axis=0)[:, :slab_rows].reshape(-1, 1)

    start = start.reshape(slab_rows, row_count, col_count // row_count).swapaxes(0, 1)
    high = lax.reduce_precision(start, 8, 7)
    low = (start - high).astype(jnp.bfloat16)
    merged, residual = solve(row_count, high.astype(jnp.bfloat16), low, total, diag)

    def placed(array):
        return array.swapaxes(0, 1).reshape(slab_rows, col_count).astype(jnp.float32)

    return placed(merged), placed(residual)


def solution(mesh):
    placed = (P(None, "row", "col"), P(None, "row", "col"))
    return jax.shard_map(
        functools.partial(shards, mesh.shape["row"], mesh.shape["col"]),
        mesh=mesh,
        in_specs=placed,
        out_specs=(P("row", "col"), P("row", "col")),
        check_vma=False,
    )
```

```python
import functools

import jax
import jax.numpy as jnp
from jax import lax
from jax.experimental import pallas as pl
from jax.experimental.pallas import tpu as pltpu
from jax.sharding import PartitionSpec as P

ITERS = 2
MESH = pl.DeviceIdType.MESH
VMEM_BYTES = 63 * 2**20


def ring_position(index, n):
    odd = index % 2
    return (1 - odd) * (index // 2) + odd * (n - 1 - index // 2)


def ring_index(position, n):
    back = position // (n // 2)
    return (1 - back) * 2 * position + back * (2 * (n - 1 - position) + 1)


def remote(source, target, send, recv, where):
    return pltpu.make_async_remote_copy(
        src_ref=source, dst_ref=target, send_sem=send, recv_sem=recv, device_id=where, device_id_type=MESH
    )


def reduce_kernel(
    n, parts, gt_ref, w_ref, slab_ref, d_ref, out_ref, t_ref, dt_ref,
    gt, sent, came, part, e_block, dg_out, dg_in, d_ring,
    g_own, g_send, g_recv, r_send, r_recv, t_own, t_send, t_recv, td_send, td_recv,
    x_send, x_recv, f_send, f_recv, dc_send, dc_recv, dg_send, dg_recv,
):
    f32, bf16 = jnp.float32, jnp.bfloat16
    row, col = lax.axis_index("row"), lax.axis_index("col")
    place = ring_position(row, n)
    chips, hops = parts // 2, n // 2
    chip, core = col // 2, col % 2
    rows, slab_cols = slab_ref.shape
    q = w_ref.shape[2]
    span = 2 * slab_cols
    half = span // 2
    cut = rows // 32 * 16
    twin = {"col": chip * 2 + 1 - core}

    def at(distance):
        return ring_index((place + n + distance) % n, n)

    right, left = {"row": at(1)}, {"row": at(-1)}

    def peer(k):
        return {"col": (chip + k) % chips * 2 + core}

    def cols_of(c):
        return pl.ds(pl.multiple_of(c * slab_cols, 16), slab_cols)

    def block(i):
        return pl.ds(pl.multiple_of(i * rows, 16), rows)

    barrier = pltpu.get_barrier_semaphore()
    for k in range(1, n):
        pl.semaphore_signal(barrier, inc=1, device_id={"row": (row + k) % n}, device_id_type=MESH)
    for k in range(1, parts):
        pl.semaphore_signal(barrier, inc=1, device_id={"col": (col + k) % parts}, device_id_type=MESH)
    own_gt = pltpu.make_async_copy(gt_ref, gt.at[cols_of(col), :], g_own)
    own_gt.start()
    own_slab = pltpu.make_async_copy(slab_ref, t_ref.at[col, row], t_own)
    own_slab.start()
    d_ring[row] = d_ref[...]
    zeros = jnp.zeros((half, q), bf16)
    came[0, 0, half:, :] = zeros
    came[1, 0, :half, :] = zeros
    pl.semaphore_wait(barrier, n - 1 + parts - 1)

    def gram_send(k):
        return remote(gt_ref, gt.at[cols_of(col), :], g_send.at[k], g_recv.at[k], peer(k) if k else twin)

    def gram_forward(k):
        origin = gt.at[cols_of((chip + chips - k) % chips * 2 + core), :]
        return remote(origin, origin, g_send.at[chips + k - 1], g_recv.at[chips + k - 1], twin)

    for k in range(chips):
        gram_send(k).start()

    def slab_hop(side, hop, kind):
        owner = at(1 - hop) if side == 0 else at(hop - 1)
        held = t_ref.at[col, owner]
        if kind == "half":
            held = t_ref.at[col, owner, pl.ds(0, cut), :] if side == 0 else t_ref.at[col, owner, pl.ds(cut, rows - cut), :]
        source = slab_ref if kind == "own" else held
        to = left if side else right
        return remote(source, held, t_send.at[side, hop - 1], t_recv.at[side, hop - 1], to)

    def diag_hop(side, hop):
        held = d_ring.at[at(1 - hop) if side == 0 else at(hop - 1)]
        return remote(held, held, td_send.at[side, hop - 1], td_recv.at[side, hop - 1], left if side else right)

    def slab_start(hop, kind):
        for side in range(2):
            slab_hop(side, hop, kind).start()
            if kind != "half" or side == 0:
                diag_hop(side, hop).start()

    def slab_wait(hop, kind):
        for side in range(2):
            slab_hop(side, hop, kind).wait()
            if kind != "half" or side == 0:
                diag_hop(side, hop).wait()

    def item(t):
        return t_ref.at[col, at((1 - 2 * (t % 2)) * ((t + 1) // 2))]

    def item_send(k, t):
        return remote(item(t), item(t), x_send.at[k, t], x_recv.at[k, t], peer(k) if k else twin)

    def item_forward(k, t):
        origin = (chip + chips - k) % chips * 2 + core
        held = t_ref.at[origin, at((1 - 2 * (t % 2)) * ((t + 1) // 2))]
        return remote(held, held, f_send.at[k - 1, t], f_recv.at[k - 1, t], twin)

    def share(t):
        for k in list(range(1, chips)) + [0]:
            item_send(k, t).start()

    def forward(t):
        for k in range(1, chips):
            item_send(k, t).wait_recv()
            item_forward(k, t).start()

    def partial(side, target, base):
        def step(i, carry):
            here = pl.ds(pl.multiple_of(base + i * rows, 16), rows)
            part[side, block(i), :] = jnp.dot(gt[here, :], w_ref[target], preferred_element_type=f32)
            return carry

        lax.fori_loop(0, span // rows, step, 0)

    def ring_hop(phase, side, hop, window):
        return remote(
            sent.at[side, hop - 1, window, :],
            came.at[side, hop - 1, window, :],
            r_send.at[phase, side, hop - 1],
            r_recv.at[phase, side, hop - 1],
            left if side else right,
        )

    halves = (pl.ds(0, half), pl.ds(half, span - half))
    whole = pl.ds(0, span)

    def diag_out(k):
        other = (row + k) % n
        for kind in range(2):
            yield remote(
                dg_out.at[kind, k],
                dg_in.at[kind, block(row), :],
                dg_send.at[kind, k],
                dg_recv.at[kind, k],
                {"row": other},
            )

    def diag_term(target):
        value = jnp.dot(e_block[...], w_ref[target], preferred_element_type=f32)
        high = value.astype(bf16)
        return high, (value - high.astype(f32)).astype(bf16)

    def diag_send(k):
        dg_out[0, k], dg_out[1, k] = diag_term((row + k) % n)
        for copy in diag_out(k):
            copy.start()

    def beside(phase, hop):
        if phase == 0:
            if isinstance(hop, int):
                slab_start(1, "own")
                own_slab.wait()
                share(0)
            else:
                slab_wait(hop - 1, "full")

                @pl.when(hop < hops)
                def _():
                    slab_start(hop, "full")

                @pl.when(hop == hops)
                def _():
                    slab_start(hops, "half")

                share(2 * (hop - 1) - 1)
                share(2 * (hop - 1))
        if phase == chips - 1:
            for k in (2 * hop - 1, 2 * hop):

                @pl.when(k < n)
                def _(k=k):
                    diag_send(k)

            if chips > 1:
                forward(2 * hop - 2)
                forward(2 * hop - 1)

    for phase in range(chips):
        source = (chip + phase) % chips
        base = source * span
        if phase == 0:
            own_gt.wait()
            gram_send(0).wait_recv()
        else:
            gram_send(phase).wait_recv()
            gram_forward(phase).start()
            gram_forward(phase).wait()

        @pl.when(row * rows // span == source)
        def _():
            mine = gt[block(row), :]
            lanes = lax.broadcasted_iota(jnp.int32, mine.shape, 1)
            below = lanes - lax.broadcasted_iota(jnp.int32, mine.shape, 0)
            chosen = below == 0
            for model in range(1, mine.shape[1] // rows):
                chosen = chosen | (below == model * rows)
            e_block[...] = jnp.where(chosen, mine.astype(f32), 0.0).astype(bf16)
            gt[block(row), :] = jnp.where(chosen, 0.0, mine.astype(f32)).astype(bf16)

        partial(0, at(hops), base)
        for side in range(2):
            if phase > 0:
                ring_hop(phase - 1, side, 1, halves[side]).wait_send()
            sent[side, 0, halves[side], :] = part[0, halves[side], :].astype(bf16)
            ring_hop(phase, side, 1, halves[side]).start()
        beside(phase, 1)

        def hop_step(hop, carry, phase=phase, base=base):
            def side_partial(side, carry):
                distance = (1 - 2 * side) * (hops + 1 - hop)
                partial(side, at(distance), base)
                return carry

            lax.fori_loop(0, 2, side_partial, 0)
            for side in range(2):

                @pl.when(hop == 2)
                def _(side=side):
                    ring_hop(phase, side, 1, halves[side]).wait_recv()

                @pl.when(hop > 2)
                def _(side=side):
                    ring_hop(phase, side, hop - 1, whole).wait_recv()

                if phase > 0:
                    ring_hop(phase - 1, side, hop, whole).wait_send()

                def add(i, carry, side=side):
                    value = part[side, block(i), :] + came[side, hop - 2, block(i), :].astype(f32)
                    sent[side, hop - 1, block(i), :] = value.astype(bf16)
                    return carry

                lax.fori_loop(0, span // rows, add, 0)
                ring_hop(phase, side, hop, whole).start()
            beside(phase, hop)
            return carry

        lax.fori_loop(2, hops + 1, hop_step, 0)
        partial(0, row, base)
        for side in range(2):
            ring_hop(phase, side, hops, whole).wait_recv()

        def close(i, carry, base=base):
            value = part[0, block(i), :]
            for side in range(2):
                value += came[side, hops - 1, block(i), :].astype(f32)
            out_ref[pl.ds(pl.multiple_of(base + i * rows, 16), rows), :] = value
            return carry

        lax.fori_loop(0, span // rows, close, 0)
        if phase == 0:
            slab_wait(hops, "half")
            share(n - 1)
            dt_ref[col] = d_ring[...]
            for k in range(1, parts):
                remote(d_ring, dt_ref.at[col], dc_send.at[k], dc_recv.at[k], {"col": (col + k) % parts}).start()

    dg_in[0, block(row), :], dg_in[1, block(row), :] = diag_term(row)

    def diag_wait(k, carry):
        for copy in diag_out(k):
            copy.wait()
        return carry

    lax.fori_loop(1, n, diag_wait, 0)

    def scale(i, carry):
        here = block(i)
        out_ref[here, :] = 0.9 * out_ref[here, :] + (dg_in[0, here, :].astype(f32) + dg_in[1, here, :].astype(f32))
        return carry

    lax.fori_loop(0, n, scale, 0)

    last = chips - 1
    for side in range(2):
        ring_hop(last, side, 1, halves[side]).wait_send()

        def sent_out(hop, carry, side=side):
            ring_hop(last, side, hop, whole).wait_send()
            return carry

        lax.fori_loop(2, hops + 1, sent_out, 0)
    for k in range(chips):
        gram_send(k).wait_send()
    for k in range(1, parts):
        remote(d_ring, dt_ref.at[col], dc_send.at[k], dc_recv.at[k], {"col": (col + k) % parts}).wait()

    def shared(t, carry):
        for k in range(chips):
            item_send(k, t).wait_send()
        item_send(0, t).wait_recv()
        for k in range(1, chips):
            item_forward(k, t).wait()
        return carry

    lax.fori_loop(0, n, shared, 0)


def reduce_columns(n, parts, gt, spread, slab, diag):
    slab_cols, depth = gt.shape
    rows = slab.shape[0]
    q = spread.shape[2]
    hops, chips, span = n // 2, parts // 2, 2 * slab_cols
    f32, bf16 = jnp.float32, jnp.bfloat16
    vmem, any_space = pl.BlockSpec(memory_space=pltpu.VMEM), pl.BlockSpec(memory_space=pl.ANY)
    dma = pltpu.SemaphoreType.DMA
    both = lambda *shape: [dma(shape), dma(shape)]
    return pl.pallas_call(
        functools.partial(reduce_kernel, n, parts),
        out_shape=(
            jax.ShapeDtypeStruct((n * rows, q), f32),
            jax.ShapeDtypeStruct((parts, n, rows, slab_cols), bf16),
            jax.ShapeDtypeStruct((parts, n) + diag.shape, f32),
        ),
        in_specs=[any_space, vmem, vmem, vmem],
        out_specs=(vmem, any_space, vmem),
        scratch_shapes=[
            pltpu.VMEM((parts * slab_cols, depth), bf16),
            pltpu.VMEM((2, hops, span, q), bf16),
            pltpu.VMEM((2, hops, span, q), bf16),
            pltpu.VMEM((2, span, q), f32),
            pltpu.VMEM((rows, depth), bf16),
            pltpu.VMEM((2, n, rows, q), bf16),
            pltpu.VMEM((2, n * rows, q), bf16),
            pltpu.VMEM((n,) + diag.shape, f32),
            dma,
            *both(2 * chips),
            *both(chips, 2, hops),
            dma,
            *both(2, hops),
            *both(2, hops),
            *both(chips, n),
            *both(max(chips - 1, 1), n),
            *both(parts),
            *both(2, n),
        ],
        compiler_params=pltpu.CompilerParams(collective_id=1, has_side_effects=True, vmem_limit_bytes=VMEM_BYTES),
    )(gt, spread, slab, diag)


def solve_kernel(
    n, parts, direction, t_ref, d_ref, om_ref, or_ref,
    tv, v, residual, mapped, out_m, out_r, t_sem, send, recv,
):
    me = lax.axis_index("row")
    rows, q = om_ref.shape[1], om_ref.shape[2]
    depth = tv.shape[2]
    f32 = jnp.float32

    barrier = pltpu.get_barrier_semaphore()
    for k in range(1, n):
        pl.semaphore_signal(barrier, inc=1, device_id={"row": (me + k) % n}, device_id_type=MESH)
    loads = [pltpu.make_async_copy(t_ref.at[c], tv.at[c], t_sem.at[c]) for c in range(parts)]
    for load in loads:
        load.start()

    def block(i):
        return pl.ds(pl.multiple_of(i * rows, 16), rows)

    def product(_):
        def step(i, carry):
            here = block(i)
            total = jnp.zeros((rows, q), f32)
            for c in range(parts):
                total += jnp.dot(tv[c, here, :], v[pl.ds(c * depth, depth), :], preferred_element_type=f32)
            mapped[here, :] = 0.9 * total + d_ref[here, :] * v[here, :].astype(f32)
            return carry

        lax.fori_loop(0, n, step, 0)

    def column_sum(terms):
        def step(i, total):
            return total + jnp.sum(terms(block(i)), axis=0, keepdims=True)

        return lax.fori_loop(0, n, step, jnp.zeros((1, q), f32))

    def first(here):
        start = direction[here, :]
        v[here, :] = start.astype(jnp.bfloat16)
        return start * start

    norm = column_sum(first)
    for load in loads:
        load.wait()
    product(0)
    curvature = column_sum(lambda here: direction[here, :] * mapped[here, :])
    step_a = norm / curvature

    def second(here):
        left = direction[here, :] - step_a * mapped[here, :]
        residual[here, :] = left
        return left * left

    norm_next = column_sum(second)
    scale = norm_next / norm

    def turn(i, carry):
        here = block(i)
        v[here, :] = (residual[here, :] + scale * direction[here, :]).astype(jnp.bfloat16)
        return carry

    lax.fori_loop(0, n, turn, 0)
    product(0)
    curvature = column_sum(lambda here: (residual[here, :] + scale * direction[here, :]) * mapped[here, :])
    step_b = norm_next / curvature

    pl.semaphore_wait(barrier, n - 1)

    def leaving(k):
        i = (me + k) % n
        return [
            remote(held.at[block(i), :], target.at[me], send.at[kind, k], recv.at[kind, k], {"row": i})
            for kind, held, target in ((0, out_m, om_ref), (1, out_r, or_ref))
        ]

    def outputs(i):
        here = block(i)
        left, start = residual[here, :], direction[here, :]
        merged = step_a * start + step_b * (left + scale * start)
        return merged.astype(jnp.bfloat16), (left - step_b * mapped[here, :]).astype(jnp.bfloat16)

    def finish(k, carry):
        i = (me + k) % n
        here = block(i)
        out_m[here, :], out_r[here, :] = outputs(i)

        @pl.when(k > 1)
        def _():
            for copy in leaving(k - 1):
                copy.start()

        return carry

    lax.fori_loop(1, n, finish, 0)
    om_ref[me], or_ref[me] = outputs(me)
    for copy in leaving(n - 1):
        copy.start()

    def drain(k, carry):
        for copy in leaving(k):
            copy.wait()
        return carry

    lax.fori_loop(1, n, drain, 0)


def solve(n, start, total, diag):
    parts = total.shape[0]
    all_rows, q = start.shape
    vmem = pl.BlockSpec(memory_space=pltpu.VMEM)
    half, full = pltpu.VMEM((all_rows, q), jnp.bfloat16), pltpu.VMEM((all_rows, q), jnp.float32)
    out = jax.ShapeDtypeStruct((n, all_rows // n, q), jnp.bfloat16)
    return pl.pallas_call(
        functools.partial(solve_kernel, n, parts),
        out_shape=(out, out),
        in_specs=[vmem, pl.BlockSpec(memory_space=pl.ANY), vmem],
        out_specs=(vmem, vmem),
        scratch_shapes=[
            pltpu.VMEM(total.shape, jnp.bfloat16),
            half,
            full,
            full,
            half,
            half,
            pltpu.SemaphoreType.DMA((parts,)),
            pltpu.SemaphoreType.DMA((2, n)),
            pltpu.SemaphoreType.DMA((2, n)),
        ],
        compiler_params=pltpu.CompilerParams(collective_id=2, has_side_effects=True, vmem_limit_bytes=VMEM_BYTES),
    )(start, total, diag)


def spread_kernel(x_ref, out_ref):
    n, _, q = out_ref.shape
    for j in range(n):
        out_ref[j] = x_ref[:, j * q : (j + 1) * q]


def spread_columns(n, flat):
    rows, columns = flat.shape
    tile = rows // 7 if rows % 112 == 0 else rows
    return pl.pallas_call(
        spread_kernel,
        grid=(rows // tile,),
        out_shape=jax.ShapeDtypeStruct((n, rows, columns // n), flat.dtype),
        in_specs=[pl.BlockSpec((tile, columns), lambda i: (i, 0))],
        out_specs=pl.BlockSpec((n, tile, columns // n), lambda i: (0, i, 0)),
    )(flat)


def join_kernel(a_ref, b_ref, a_out, b_out):
    n, _, q = a_ref.shape
    for source, target in ((a_ref, a_out), (b_ref, b_out)):
        for j in range(n):
            target[:, j * q : (j + 1) * q] = source[j].astype(target.dtype)


def join_columns(a, b):
    n, rows, q = a.shape
    tile = rows // 7 if rows % 112 == 0 else rows
    out = jax.ShapeDtypeStruct((rows, n * q), jnp.float32)
    taken = pl.BlockSpec((n, tile, q), lambda i: (0, i, 0))
    given = pl.BlockSpec((tile, n * q), lambda i: (i, 0))
    return pl.pallas_call(
        join_kernel, grid=(rows // tile,), out_shape=(out, out), in_specs=[taken, taken], out_specs=(given, given)
    )(a, b)


def shards(n, parts, grams, weights):
    models, rows, slab_cols = grams.shape

    own_total = jnp.sum(grams.astype(jnp.float32), axis=0)
    row_ids = lax.axis_index("row") * rows + jnp.arange(rows)[:, None]
    col_ids = lax.axis_index("col") * slab_cols + jnp.arange(slab_cols)[None, :]
    diagonal = row_ids == col_ids
    slab = jnp.where(diagonal, 0.0, own_total).astype(jnp.bfloat16)
    own_diag = jnp.sum(jnp.where(diagonal, own_total, 0.0), axis=1)
    padded = -(-rows // 1024) * 1024
    own_diag = jnp.pad(own_diag, (0, padded - rows)).reshape(-1, 128)

    transposed = grams.transpose(2, 0, 1).reshape(slab_cols, models * rows)
    spread = spread_columns(n, weights.reshape(models * rows, -1))
    start, total, diag_slabs = reduce_columns(n, parts, transposed, spread, slab, own_diag)
    diag = jnp.sum(diag_slabs.reshape(parts, n, padded), axis=0)[:, :rows].reshape(-1, 1)
    merged, residual = solve(n, start, total.reshape(parts, n * rows, slab_cols), diag)
    return join_columns(merged, residual)


def solution(mesh):
    placed = (P(None, "row", "col"), P(None, "row", "col"))
    return jax.shard_map(
        functools.partial(shards, mesh.shape["row"], mesh.shape["col"]),
        mesh=mesh,
        in_specs=placed,
        out_specs=(P("row", "col"), P("row", "col")),
        check_vma=False,
    )
```

```python
import functools

import jax
import jax.numpy as jnp
from jax import lax
from jax.experimental import pallas as pl
from jax.experimental.pallas import tpu as pltpu
from jax.sharding import PartitionSpec as P

ITERS = 2
MESH = pl.DeviceIdType.MESH
VMEM_BYTES = 63 * 2**20


def ring_position(index, n):
    odd = index % 2
    return (1 - odd) * (index // 2) + odd * (n - 1 - index // 2)


def ring_index(position, n):
    back = position // (n // 2)
    return (1 - back) * 2 * position + back * (2 * (n - 1 - position) + 1)


def remote(source, target, send, recv, where):
    return pltpu.make_async_remote_copy(
        src_ref=source, dst_ref=target, send_sem=send, recv_sem=recv, device_id=where, device_id_type=MESH
    )


def reduce_kernel(
    n, parts, gt_ref, w_ref, slab_ref, d_ref, out_ref, t_ref, dt_ref,
    gt, sent, came, part, e_block, lo_sent, lo_came, d_ring,
    g_own, g_send, g_recv, r_send, r_recv, t_own, t_send, t_recv, td_send, td_recv,
    x_send, x_recv, f_send, f_recv, dc_send, dc_recv, lo_send, lo_recv,
):
    f32, bf16 = jnp.float32, jnp.bfloat16
    row, col = lax.axis_index("row"), lax.axis_index("col")
    place = ring_position(row, n)
    chips, hops = parts // 2, n // 2
    chip, core = col // 2, col % 2
    rows, slab_cols = slab_ref.shape
    q = w_ref.shape[2]
    span = 2 * slab_cols
    half = span // 2
    cut = rows // 32 * 16
    twin = {"col": chip * 2 + 1 - core}

    def at(distance):
        return ring_index((place + n + distance) % n, n)

    right, left = {"row": at(1)}, {"row": at(-1)}

    def peer(k):
        return {"col": (chip + k) % chips * 2 + core}

    def cols_of(c):
        return pl.ds(pl.multiple_of(c * slab_cols, 16), slab_cols)

    def block(i):
        return pl.ds(pl.multiple_of(i * rows, 16), rows)

    barrier = pltpu.get_barrier_semaphore()
    for k in range(1, n):
        pl.semaphore_signal(barrier, inc=1, device_id={"row": (row + k) % n}, device_id_type=MESH)
    for k in range(1, parts):
        pl.semaphore_signal(barrier, inc=1, device_id={"col": (col + k) % parts}, device_id_type=MESH)
    own_gt = pltpu.make_async_copy(gt_ref, gt.at[cols_of(col), :], g_own)
    own_gt.start()
    own_slab = pltpu.make_async_copy(slab_ref, t_ref.at[col, row], t_own)
    own_slab.start()
    d_ring[row] = d_ref[...]
    zeros = jnp.zeros((half, q), bf16)
    came[0, 0, half:, :] = zeros
    came[1, 0, :half, :] = zeros
    pl.semaphore_wait(barrier, n - 1 + parts - 1)

    def gram_send(k):
        return remote(gt_ref, gt.at[cols_of(col), :], g_send.at[k], g_recv.at[k], peer(k) if k else twin)

    def gram_forward(k):
        origin = gt.at[cols_of((chip + chips - k) % chips * 2 + core), :]
        return remote(origin, origin, g_send.at[chips + k - 1], g_recv.at[chips + k - 1], twin)

    for k in range(chips):
        gram_send(k).start()

    def slab_hop(side, hop, kind):
        owner = at(1 - hop) if side == 0 else at(hop - 1)
        held = t_ref.at[col, owner]
        if kind == "half":
            held = t_ref.at[col, owner, pl.ds(0, cut), :] if side == 0 else t_ref.at[col, owner, pl.ds(cut, rows - cut), :]
        source = slab_ref if kind == "own" else held
        to = left if side else right
        return remote(source, held, t_send.at[side, hop - 1], t_recv.at[side, hop - 1], to)

    def diag_hop(side, hop):
        held = d_ring.at[at(1 - hop) if side == 0 else at(hop - 1)]
        return remote(held, held, td_send.at[side, hop - 1], td_recv.at[side, hop - 1], left if side else right)

    def slab_start(hop, kind):
        for side in range(2):
            slab_hop(side, hop, kind).start()
            if kind != "half" or side == 0:
                diag_hop(side, hop).start()

    def slab_wait(hop, kind):
        for side in range(2):
            slab_hop(side, hop, kind).wait()
            if kind != "half" or side == 0:
                diag_hop(side, hop).wait()

    def item(t):
        return t_ref.at[col, at((1 - 2 * (t % 2)) * ((t + 1) // 2))]

    def item_send(k, t):
        return remote(item(t), item(t), x_send.at[k, t], x_recv.at[k, t], peer(k) if k else twin)

    def item_forward(k, t):
        origin = (chip + chips - k) % chips * 2 + core
        held = t_ref.at[origin, at((1 - 2 * (t % 2)) * ((t + 1) // 2))]
        return remote(held, held, f_send.at[k - 1, t], f_recv.at[k - 1, t], twin)

    def share(t):
        for k in list(range(1, chips)) + [0]:
            item_send(k, t).start()

    def forward(t):
        for k in range(1, chips):
            item_send(k, t).wait_recv()
            item_forward(k, t).start()

    def partial(side, target, base):
        def step(i, carry):
            here = pl.ds(pl.multiple_of(base + i * rows, 16), rows)
            part[side, block(i), :] = jnp.dot(gt[here, :], w_ref[target], preferred_element_type=f32)
            return carry

        lax.fori_loop(0, span // rows, step, 0)

    def ring_hop(phase, side, hop, window):
        return remote(
            sent.at[side, hop - 1, window, :],
            came.at[side, hop - 1, window, :],
            r_send.at[phase, side, hop - 1],
            r_recv.at[phase, side, hop - 1],
            left if side else right,
        )

    halves = (pl.ds(0, half), pl.ds(half, span - half))
    whole = pl.ds(0, span)

    def slot(hop, u):
        return hop * (hop - 1) // 2 + u

    def low_hop(side, hop, u):
        here = slot(hop, u)
        return remote(
            lo_sent.at[side, here],
            lo_came.at[side, here],
            lo_send.at[side, here],
            lo_recv.at[side, here],
            left if side else right,
        )

    def member(side, u):
        return at((2 * side - 1) * u)

    def carried(side, hop, u, source, shift):
        first = member(side, u + shift) * rows
        used = (u < hop - 1) | ((first % span) // half == side)
        return used if source is None else used & (first // span == source)

    def diag_term(target):
        return jnp.dot(e_block[...], w_ref[target], preferred_element_type=f32) * (1 / 9)

    def beside(phase, hop):
        if phase == 0:
            if isinstance(hop, int):
                slab_start(1, "own")
                own_slab.wait()
                share(0)
            else:
                slab_wait(hop - 1, "full")

                @pl.when(hop < hops)
                def _():
                    slab_start(hop, "full")

                @pl.when(hop == hops)
                def _():
                    slab_start(hops, "half")

                share(2 * (hop - 1) - 1)
                share(2 * (hop - 1))
        if phase == chips - 1 and chips > 1:
            forward(2 * hop - 2)
            forward(2 * hop - 1)

    for phase in range(chips):
        source = (chip + phase) % chips
        base = source * span
        if phase == 0:
            own_gt.wait()
            gram_send(0).wait_recv()
        else:
            gram_send(phase).wait_recv()
            gram_forward(phase).start()
            gram_forward(phase).wait_recv()

        @pl.when(row * rows // span == source)
        def _():
            mine = gt[block(row), :]
            lanes = lax.broadcasted_iota(jnp.int32, mine.shape, 1)
            below = lanes - lax.broadcasted_iota(jnp.int32, mine.shape, 0)
            chosen = below == 0
            for model in range(1, mine.shape[1] // rows):
                chosen = chosen | (below == model * rows)
            e_block[...] = jnp.where(chosen, mine.astype(f32), 0.0).astype(bf16)

        partial(0, at(hops), base)
        for side in range(2):
            if phase > 0:
                ring_hop(phase - 1, side, 1, halves[side]).wait_send()
            sent[side, 0, halves[side], :] = part[0, halves[side], :].astype(bf16)

            @pl.when(carried(side, 1, 0, source, 0))
            def _(side=side, base=base):
                here = pl.ds(pl.multiple_of(row * rows - base, 16), rows)
                value = part[0, here, :] + diag_term(at(hops))
                high = value.astype(bf16)
                sent[side, 0, here, :] = high
                lo_sent[side, 0] = (value - high.astype(f32)).astype(bf16)
                low_hop(side, 1, 0).start()

            ring_hop(phase, side, 1, halves[side]).start()
        beside(phase, 1)

        def hop_step(hop, carry, phase=phase, base=base, source=source):
            def side_partial(side, carry):
                distance = (1 - 2 * side) * (hops + 1 - hop)
                partial(side, at(distance), base)
                return carry

            lax.fori_loop(0, 2, side_partial, 0)
            for side in range(2):

                @pl.when(hop == 2)
                def _(side=side):
                    ring_hop(phase, side, 1, halves[side]).wait_recv()

                @pl.when(hop > 2)
                def _(side=side):
                    ring_hop(phase, side, hop - 1, whole).wait_recv()

                if phase > 0:
                    ring_hop(phase - 1, side, hop, whole).wait_send()

                def add(i, carry, side=side):
                    value = part[side, block(i), :] + came[side, hop - 2, block(i), :].astype(f32)
                    sent[side, hop - 1, block(i), :] = value.astype(bf16)
                    return carry

                lax.fori_loop(0, span // rows, add, 0)
                for u in range(hops):

                    @pl.when((u < hop) & carried(side, hop, u, source, 0))
                    def _(side=side, u=u):
                        here = pl.ds(pl.multiple_of(member(side, u) * rows - base, 16), rows)
                        value = part[side, here, :] + came[side, hop - 2, here, :].astype(f32)
                        if u == 0:
                            value += diag_term(at((1 - 2 * side) * (hops + 1 - hop)))
                        else:
                            low_hop(side, hop - 1, u - 1).wait_recv()
                            value += lo_came[side, slot(hop - 1, u - 1)].astype(f32)
                        high = value.astype(bf16)
                        sent[side, hop - 1, here, :] = high
                        lo_sent[side, slot(hop, u)] = (value - high.astype(f32)).astype(bf16)
                        low_hop(side, hop, u).start()

                ring_hop(phase, side, hop, whole).start()
            beside(phase, hop)
            return carry

        lax.fori_loop(2, hops + 1, hop_step, 0)
        partial(0, row, base)
        for side in range(2):
            ring_hop(phase, side, hops, whole).wait_recv()

        def close(i, carry, base=base):
            value = part[0, block(i), :]
            for side in range(2):
                value += came[side, hops - 1, block(i), :].astype(f32)
            out_ref[pl.ds(pl.multiple_of(base + i * rows, 16), rows), :] = 0.9 * value
            return carry

        lax.fori_loop(0, span // rows, close, 0)

        @pl.when(row * rows // span == source)
        def _():
            out_ref[block(row), :] += 0.9 * diag_term(row)

        for side in range(2):
            for u in range(hops):

                @pl.when(carried(side, hops, u, source, 1))
                def _(side=side, u=u):
                    low_hop(side, hops, u).wait_recv()
                    out_ref[block(member(side, u + 1)), :] += 0.9 * lo_came[side, slot(hops, u)].astype(f32)

        if phase == 0:
            slab_wait(hops, "half")
            share(n - 1)
            dt_ref[col] = d_ring[...]
            for k in range(1, parts):
                remote(d_ring, dt_ref.at[col], dc_send.at[k], dc_recv.at[k], {"col": (col + k) % parts}).start()

    last = chips - 1
    for side in range(2):
        ring_hop(last, side, 1, halves[side]).wait_send()

        def sent_out(hop, carry, side=side):
            ring_hop(last, side, hop, whole).wait_send()
            return carry

        lax.fori_loop(2, hops + 1, sent_out, 0)

        def low_out(hop, carry, side=side):
            for u in range(hops):

                @pl.when((u < hop) & carried(side, hop, u, None, 0))
                def _(u=u):
                    low_hop(side, hop, u).wait_send()

            return carry

        lax.fori_loop(1, hops + 1, low_out, 0)
    for k in range(chips):
        gram_send(k).wait_send()
    for k in range(1, chips):
        gram_forward(k).wait_send()
    for k in range(1, parts):
        remote(d_ring, dt_ref.at[col], dc_send.at[k], dc_recv.at[k], {"col": (col + k) % parts}).wait()

    def shared(t, carry):
        for k in range(chips):
            item_send(k, t).wait_send()
        item_send(0, t).wait_recv()
        for k in range(1, chips):
            item_forward(k, t).wait()
        return carry

    lax.fori_loop(0, n, shared, 0)


def reduce_columns(n, parts, gt, spread, slab, diag):
    slab_cols, depth = gt.shape
    rows = slab.shape[0]
    q = spread.shape[2]
    hops, chips, span = n // 2, parts // 2, 2 * slab_cols
    slots = hops * (hops + 1) // 2
    f32, bf16 = jnp.float32, jnp.bfloat16
    vmem, any_space = pl.BlockSpec(memory_space=pltpu.VMEM), pl.BlockSpec(memory_space=pl.ANY)
    dma = pltpu.SemaphoreType.DMA
    both = lambda *shape: [dma(shape), dma(shape)]
    return pl.pallas_call(
        functools.partial(reduce_kernel, n, parts),
        out_shape=(
            jax.ShapeDtypeStruct((n * rows, q), f32),
            jax.ShapeDtypeStruct((parts, n, rows, slab_cols), bf16),
            jax.ShapeDtypeStruct((parts, n) + diag.shape, f32),
        ),
        in_specs=[any_space, vmem, vmem, vmem],
        out_specs=(vmem, any_space, vmem),
        scratch_shapes=[
            pltpu.VMEM((parts * slab_cols, depth), bf16),
            pltpu.VMEM((2, hops, span, q), bf16),
            pltpu.VMEM((2, hops, span, q), bf16),
            pltpu.VMEM((2, span, q), f32),
            pltpu.VMEM((rows, depth), bf16),
            pltpu.VMEM((2, slots, rows, q), bf16),
            pltpu.VMEM((2, slots, rows, q), bf16),
            pltpu.VMEM((n,) + diag.shape, f32),
            dma,
            *both(2 * chips),
            *both(chips, 2, hops),
            dma,
            *both(2, hops),
            *both(2, hops),
            *both(chips, n),
            *both(max(chips - 1, 1), n),
            *both(parts),
            *both(2, slots),
        ],
        compiler_params=pltpu.CompilerParams(collective_id=1, has_side_effects=True, vmem_limit_bytes=VMEM_BYTES),
    )(gt, spread, slab, diag)


def solve_kernel(
    n, parts, direction, t_ref, d_ref, om_ref, or_ref,
    tv, v, residual, mapped, out_m, out_r, t_sem, send, recv,
):
    me = lax.axis_index("row")
    rows, q = om_ref.shape[1], om_ref.shape[2]
    depth = tv.shape[3]
    f32 = jnp.float32

    barrier = pltpu.get_barrier_semaphore()
    for k in range(1, n):
        pl.semaphore_signal(barrier, inc=1, device_id={"row": (me + k) % n}, device_id_type=MESH)

    def load(i):
        return pltpu.make_async_copy(t_ref.at[:, i], tv.at[i], t_sem.at[i])

    for i in range(n):
        load(i).start()

    def block(i):
        return pl.ds(pl.multiple_of(i * rows, 16), rows)

    def product(loading):
        def step(i, carry):
            if loading:
                load(i).wait()
            here = block(i)
            total = jnp.zeros((rows, q), f32)
            for c in range(parts):
                total += jnp.dot(tv[i, c], v[pl.ds(c * depth, depth), :], preferred_element_type=f32)
            mapped[here, :] = 0.9 * total + d_ref[here, :] * v[here, :].astype(f32)
            return carry

        lax.fori_loop(0, n, step, 0)

    def column_sum(terms):
        def step(i, total):
            return total + jnp.sum(terms(block(i)), axis=0, keepdims=True)

        return lax.fori_loop(0, n, step, jnp.zeros((1, q), f32))

    def first(here):
        start = direction[here, :]
        v[here, :] = start.astype(jnp.bfloat16)
        return start * start

    norm = column_sum(first)
    product(True)
    curvature = column_sum(lambda here: direction[here, :] * mapped[here, :])
    step_a = norm / curvature

    def second(here):
        left = direction[here, :] - step_a * mapped[here, :]
        residual[here, :] = left
        return left * left

    norm_next = column_sum(second)
    scale = norm_next / norm

    def turn(i, carry):
        here = block(i)
        v[here, :] = (residual[here, :] + scale * direction[here, :]).astype(jnp.bfloat16)
        return carry

    lax.fori_loop(0, n, turn, 0)
    product(False)
    curvature = column_sum(lambda here: (residual[here, :] + scale * direction[here, :]) * mapped[here, :])
    step_b = norm_next / curvature

    pl.semaphore_wait(barrier, n - 1)

    def leaving(k):
        i = (me + k) % n
        return [
            remote(held.at[block(i), :], target.at[me], send.at[kind, k], recv.at[kind, k], {"row": i})
            for kind, held, target in ((0, out_m, om_ref), (1, out_r, or_ref))
        ]

    def outputs(i):
        here = block(i)
        left, start = residual[here, :], direction[here, :]
        merged = step_a * start + step_b * (left + scale * start)
        return merged.astype(jnp.bfloat16), (left - step_b * mapped[here, :]).astype(jnp.bfloat16)

    def finish(k, carry):
        i = (me + k) % n
        here = block(i)
        out_m[here, :], out_r[here, :] = outputs(i)

        @pl.when(k > 1)
        def _():
            for copy in leaving(k - 1):
                copy.start()

        return carry

    lax.fori_loop(1, n, finish, 0)
    om_ref[me], or_ref[me] = outputs(me)
    for copy in leaving(n - 1):
        copy.start()

    def drain(k, carry):
        for copy in leaving(k):
            copy.wait()
        return carry

    lax.fori_loop(1, n, drain, 0)


def solve(n, start, total, diag):
    parts = total.shape[0]
    all_rows, q = start.shape
    vmem = pl.BlockSpec(memory_space=pltpu.VMEM)
    half, full = pltpu.VMEM((all_rows, q), jnp.bfloat16), pltpu.VMEM((all_rows, q), jnp.float32)
    out = jax.ShapeDtypeStruct((n, all_rows // n, q), jnp.bfloat16)
    return pl.pallas_call(
        functools.partial(solve_kernel, n, parts),
        out_shape=(out, out),
        in_specs=[vmem, pl.BlockSpec(memory_space=pl.ANY), vmem],
        out_specs=(vmem, vmem),
        scratch_shapes=[
            pltpu.VMEM((n, parts) + total.shape[2:], jnp.bfloat16),
            half,
            full,
            full,
            half,
            half,
            pltpu.SemaphoreType.DMA((n,)),
            pltpu.SemaphoreType.DMA((2, n)),
            pltpu.SemaphoreType.DMA((2, n)),
        ],
        compiler_params=pltpu.CompilerParams(collective_id=2, has_side_effects=True, vmem_limit_bytes=VMEM_BYTES),
    )(start, total, diag)


def spread_kernel(x_ref, out_ref):
    n, _, q = out_ref.shape
    for j in range(n):
        out_ref[j] = x_ref[:, j * q : (j + 1) * q]


def spread_columns(n, flat):
    rows, columns = flat.shape
    tile = rows // 7 if rows % 112 == 0 else rows
    return pl.pallas_call(
        spread_kernel,
        grid=(rows // tile,),
        out_shape=jax.ShapeDtypeStruct((n, rows, columns // n), flat.dtype),
        in_specs=[pl.BlockSpec((tile, columns), lambda i: (i, 0))],
        out_specs=pl.BlockSpec((n, tile, columns // n), lambda i: (0, i, 0)),
    )(flat)


def join_kernel(a_ref, b_ref, a_out, b_out):
    n, _, q = a_ref.shape
    for source, target in ((a_ref, a_out), (b_ref, b_out)):
        for j in range(n):
            target[:, j * q : (j + 1) * q] = source[j].astype(target.dtype)


def join_columns(a, b):
    n, rows, q = a.shape
    tile = rows // 7 if rows % 112 == 0 else rows
    out = jax.ShapeDtypeStruct((rows, n * q), jnp.float32)
    taken = pl.BlockSpec((n, tile, q), lambda i: (0, i, 0))
    given = pl.BlockSpec((tile, n * q), lambda i: (i, 0))
    return pl.pallas_call(
        join_kernel, grid=(rows // tile,), out_shape=(out, out), in_specs=[taken, taken], out_specs=(given, given)
    )(a, b)


def shards(n, parts, grams, weights):
    models, rows, slab_cols = grams.shape

    own_total = jnp.sum(grams.astype(jnp.float32), axis=0)
    row_ids = lax.axis_index("row") * rows + jnp.arange(rows)[:, None]
    col_ids = lax.axis_index("col") * slab_cols + jnp.arange(slab_cols)[None, :]
    diagonal = row_ids == col_ids
    slab = jnp.where(diagonal, 0.0, own_total).astype(jnp.bfloat16)
    own_diag = jnp.sum(jnp.where(diagonal, own_total, 0.0), axis=1)
    padded = -(-rows // 1024) * 1024
    own_diag = jnp.pad(own_diag, (0, padded - rows)).reshape(-1, 128)

    transposed = grams.transpose(2, 0, 1).reshape(slab_cols, models * rows)
    spread = spread_columns(n, weights.reshape(models * rows, -1))
    start, total, diag_slabs = reduce_columns(n, parts, transposed, spread, slab, own_diag)
    diag = jnp.sum(diag_slabs.reshape(parts, n, padded), axis=0)[:, :rows].reshape(-1, 1)
    merged, residual = solve(n, start, total, diag)
    return join_columns(merged, residual)


def solution(mesh):
    placed = (P(None, "row", "col"), P(None, "row", "col"))
    return jax.shard_map(
        functools.partial(shards, mesh.shape["row"], mesh.shape["col"]),
        mesh=mesh,
        in_specs=placed,
        out_specs=(P("row", "col"), P("row", "col")),
        check_vma=False,
    )
```

```python
import functools

import jax
import jax.numpy as jnp
from jax import lax
from jax.experimental import pallas as pl
from jax.experimental.pallas import tpu as pltpu
from jax.sharding import PartitionSpec as P

ITERS = 2
MESH = pl.DeviceIdType.MESH
VMEM_BYTES = 63 * 2**20


def ring_position(index, n):
    odd = index % 2
    return (1 - odd) * (index // 2) + odd * (n - 1 - index // 2)


def ring_index(position, n):
    back = position // (n // 2)
    return (1 - back) * 2 * position + back * (2 * (n - 1 - position) + 1)


def remote(source, target, send, recv, where):
    return pltpu.make_async_remote_copy(
        src_ref=source, dst_ref=target, send_sem=send, recv_sem=recv, device_id=where, device_id_type=MESH
    )


def reduce_kernel(
    n, parts, gt_ref, flat_ref, slab_ref, d_ref, out_ref, t_ref, dt_ref,
    w_ref, staged, gt, sent, came, part, e_block, lo_sent, lo_came, d_ring,
    w_sem, g_own, g_send, g_recv, r_send, r_recv, t_own, t_send, t_recv, td_send, td_recv,
    x_send, x_recv, f_send, f_recv, dc_send, dc_recv, lo_send, lo_recv,
):
    f32, bf16 = jnp.float32, jnp.bfloat16
    row, col = lax.axis_index("row"), lax.axis_index("col")
    place = ring_position(row, n)
    chips, hops = parts // 2, n // 2
    chip, core = col // 2, col % 2
    rows, slab_cols = slab_ref.shape
    q = out_ref.shape[1]
    span = 2 * slab_cols
    half = span // 2
    cut = rows // 32 * 16
    twin = {"col": chip * 2 + 1 - core}

    def at(distance):
        return ring_index((place + n + distance) % n, n)

    right, left = {"row": at(1)}, {"row": at(-1)}

    def peer(k):
        return {"col": (chip + k) % chips * 2 + core}

    def cols_of(c):
        return pl.ds(pl.multiple_of(c * slab_cols, 16), slab_cols)

    def block(i):
        return pl.ds(pl.multiple_of(i * rows, 16), rows)

    barrier = pltpu.get_barrier_semaphore()
    for k in range(1, n):
        pl.semaphore_signal(barrier, inc=1, device_id={"row": (row + k) % n}, device_id_type=MESH)
    for k in range(1, parts):
        pl.semaphore_signal(barrier, inc=1, device_id={"col": (col + k) % parts}, device_id_type=MESH)
    own_gt = pltpu.make_async_copy(gt_ref, gt.at[cols_of(col), :], g_own)
    own_gt.start()
    own_slab = pltpu.make_async_copy(slab_ref, t_ref.at[col, row], t_own)
    own_slab.start()
    d_ring[row] = d_ref[...]
    zeros = jnp.zeros((half, q), bf16)
    for k in range(chips):
        came[0, 0, k, half:, :] = zeros
        came[1, 0, k, :half, :] = zeros
    pl.semaphore_wait(barrier, n - 1 + parts - 1)

    def gram_send(k):
        return remote(gt_ref, gt.at[cols_of(col), :], g_send.at[k], g_recv.at[k], peer(k) if k else twin)

    def gram_forward(k):
        origin = gt.at[cols_of((chip + chips - k) % chips * 2 + core), :]
        return remote(origin, origin, g_send.at[chips + k - 1], g_recv.at[chips + k - 1], twin)

    for k in range(chips):
        gram_send(k).start()

    def slab_hop(side, hop, kind):
        owner = at(1 - hop) if side == 0 else at(hop - 1)
        held = t_ref.at[col, owner]
        if kind == "half":
            held = t_ref.at[col, owner, pl.ds(0, cut), :] if side == 0 else t_ref.at[col, owner, pl.ds(cut, rows - cut), :]
        source = slab_ref if kind == "own" else held
        to = left if side else right
        return remote(source, held, t_send.at[side, hop - 1], t_recv.at[side, hop - 1], to)

    def diag_hop(side, hop):
        held = d_ring.at[at(1 - hop) if side == 0 else at(hop - 1)]
        return remote(held, held, td_send.at[side, hop - 1], td_recv.at[side, hop - 1], left if side else right)

    def slab_start(hop, kind):
        for side in range(2):
            slab_hop(side, hop, kind).start()
            if kind != "half" or side == 0:
                diag_hop(side, hop).start()

    def slab_wait(hop, kind):
        for side in range(2):
            slab_hop(side, hop, kind).wait()
            if kind != "half" or side == 0:
                diag_hop(side, hop).wait()

    def item(t):
        return t_ref.at[col, at((1 - 2 * (t % 2)) * ((t + 1) // 2))]

    def item_send(k, t):
        return remote(item(t), item(t), x_send.at[k, t], x_recv.at[k, t], peer(k) if k else twin)

    def item_forward(k, t):
        origin = (chip + chips - k) % chips * 2 + core
        held = t_ref.at[origin, at((1 - 2 * (t % 2)) * ((t + 1) // 2))]
        return remote(held, held, f_send.at[k - 1, t], f_recv.at[k - 1, t], twin)

    def share(t):
        for k in list(range(1, chips)) + [0]:
            item_send(k, t).start()

    def forward(t):
        for k in range(1, chips):
            item_send(k, t).wait_recv()
            item_forward(k, t).start()

    def partial(side, target, base):
        def step(i, carry):
            here = pl.ds(pl.multiple_of(base + i * rows, 16), rows)
            part[side, block(i), :] = jnp.dot(gt[here, :], w_ref[target], preferred_element_type=f32)
            return carry

        lax.fori_loop(0, span // rows, step, 0)

    def ring_hop(k, side, hop, window):
        slot_of = (hop - 1) % 2
        return remote(
            sent.at[side, slot_of, k, window, :],
            came.at[side, slot_of, k, window, :],
            r_send.at[k, side, hop - 1],
            r_recv.at[k, side, hop - 1],
            left if side else right,
        )

    halves = (pl.ds(0, half), pl.ds(half, span - half))
    whole = pl.ds(0, span)

    def slot(hop, u):
        return hop * (hop - 1) // 2 + u

    def low_hop(side, hop, u):
        here = slot(hop, u)
        return remote(
            lo_sent.at[side, here],
            lo_came.at[side, here],
            lo_send.at[side, here],
            lo_recv.at[side, here],
            left if side else right,
        )

    def member(side, u):
        return at((2 * side - 1) * u)

    def carried(side, hop, u, source, shift):
        first = member(side, u + shift) * rows
        used = (u < hop - 1) | ((first % span) // half == side)
        return used if source is None else used & (first // span == source)

    def diag_term(target):
        return jnp.dot(e_block[...], w_ref[target], preferred_element_type=f32) * (1 / 9)

    def source_of(k):
        return (chip + k) % chips

    def extract(k):
        @pl.when(row * rows // span == source_of(k))
        def _():
            mine = gt[block(row), :]
            lanes = lax.broadcasted_iota(jnp.int32, mine.shape, 1)
            below = lanes - lax.broadcasted_iota(jnp.int32, mine.shape, 0)
            chosen = below == 0
            for model in range(1, mine.shape[1] // rows):
                chosen = chosen | (below == model * rows)
            e_block[...] = jnp.where(chosen, mine.astype(f32), 0.0).astype(bf16)

    def split(k, side, hop, u, value):
        here = pl.ds(pl.multiple_of(member(side, u) * rows - source_of(k) * span, 16), rows)
        high = value.astype(bf16)
        sent[side, (hop - 1) % 2, k, here, :] = high
        lo_sent[side, slot(hop, u)] = (value - high.astype(f32)).astype(bf16)

    def local(k, side, u):
        return pl.ds(pl.multiple_of(member(side, u) * rows - source_of(k) * span, 16), rows)

    def first_hop(k):
        extract(k)
        partial(0, at(hops), source_of(k) * span)
        for side in range(2):
            sent[side, 0, k, halves[side], :] = part[0, halves[side], :].astype(bf16)

            @pl.when(carried(side, 1, 0, source_of(k), 0))
            def _(side=side):
                split(k, side, 1, 0, part[0, local(k, side, 0), :] + diag_term(at(hops)))

        for side in range(2):
            ring_hop(k, side, 1, halves[side]).start()

            @pl.when(carried(side, 1, 0, source_of(k), 0))
            def _(side=side):
                low_hop(side, 1, 0).start()

    def later_hop(k, hop):
        source = source_of(k)

        def side_partial(side, carry):
            partial(side, at((1 - 2 * side) * (hops + 1 - hop)), source * span)
            return carry

        lax.fori_loop(0, 2, side_partial, 0)
        for side in range(2):

            @pl.when(hop == 2)
            def _(side=side):
                ring_hop(k, side, 1, halves[side]).wait_recv()

            @pl.when(hop > 2)
            def _(side=side):
                ring_hop(k, side, hop - 1, whole).wait_recv()

            @pl.when(hop == 3)
            def _(side=side):
                ring_hop(k, side, 1, halves[side]).wait_send()

            @pl.when(hop > 3)
            def _(side=side):
                ring_hop(k, side, hop - 2, whole).wait_send()

            def add(i, carry, side=side):
                value = part[side, block(i), :] + came[side, hop % 2, k, block(i), :].astype(f32)
                sent[side, (hop - 1) % 2, k, block(i), :] = value.astype(bf16)
                return carry

            lax.fori_loop(0, span // rows, add, 0)
            for u in range(hops):

                @pl.when((u < hop) & carried(side, hop, u, source, 0))
                def _(side=side, u=u):
                    here = local(k, side, u)
                    value = part[side, here, :] + came[side, hop % 2, k, here, :].astype(f32)
                    if u == 0:
                        value += diag_term(at((1 - 2 * side) * (hops + 1 - hop)))
                    else:
                        low_hop(side, hop - 1, u - 1).wait_recv()
                        value += lo_came[side, slot(hop - 1, u - 1)].astype(f32)
                    split(k, side, hop, u, value)

        for side in range(2):
            ring_hop(k, side, hop, whole).start()
            for u in range(hops):

                @pl.when((u < hop) & carried(side, hop, u, source, 0))
                def _(side=side, u=u):
                    low_hop(side, hop, u).start()

    def close_part(k):
        source = source_of(k)
        partial(0, row, source * span)
        for side in range(2):
            ring_hop(k, side, hops, whole).wait_recv()

        def close(i, carry):
            value = part[0, block(i), :]
            for side in range(2):
                value += came[side, (hops - 1) % 2, k, block(i), :].astype(f32)
            out_ref[pl.ds(pl.multiple_of(source * span + i * rows, 16), rows), :] = 0.9 * value
            return carry

        lax.fori_loop(0, span // rows, close, 0)

        @pl.when(row * rows // span == source)
        def _():
            out_ref[block(row), :] += 0.9 * diag_term(row)

        for side in range(2):
            for u in range(hops):

                @pl.when(carried(side, hops, u, source, 1))
                def _(side=side, u=u):
                    low_hop(side, hops, u).wait_recv()
                    out_ref[block(member(side, u + 1)), :] += 0.9 * lo_came[side, slot(hops, u)].astype(f32)

    tile = staged.shape[1]
    tiles = w_ref.shape[1] // tile

    def staging(i):
        source = flat_ref.at[pl.ds(pl.multiple_of(i * tile, 16), tile), :]
        return pltpu.make_async_copy(source, staged.at[i % 2], w_sem.at[i % 2])

    def spread(i, carry):
        @pl.when(i + 1 < tiles)
        def _():
            staging(i + 1).start()

        staging(i).wait()
        for j in range(n):
            w_ref[j, pl.ds(pl.multiple_of(i * tile, 16), tile), :] = staged[i % 2, :, j * q : (j + 1) * q]
        return carry

    slab_start(1, "own")
    staging(0).start()
    own_slab.wait()
    share(0)
    lax.fori_loop(0, tiles, spread, 0)
    own_gt.wait()
    gram_send(0).wait_recv()
    first_hop(0)

    def slab_step(hop, carry):
        slab_wait(hop - 1, "full")
        slab_start(hop, "full")
        share(2 * (hop - 1) - 1)
        share(2 * (hop - 1))
        return carry

    slab_step(2, 0)
    later_hop(0, jnp.int32(2))
    lax.fori_loop(3, hops, slab_step, 0)
    slab_wait(hops - 1, "full")
    slab_start(hops, "half")
    share(n - 3)
    share(n - 2)
    for k in range(1, chips):
        gram_send(k).wait_recv()
        gram_forward(k).start()
    for k in range(1, chips):
        gram_forward(k).wait_recv()
        first_hop(k)
    slab_wait(hops, "half")
    share(n - 1)
    dt_ref[col] = d_ring[...]
    for k in range(1, parts):
        remote(d_ring, dt_ref.at[col], dc_send.at[k], dc_recv.at[k], {"col": (col + k) % parts}).start()

    def hop_step(hop, carry):
        later_hop(0, hop + 1)
        for k in range(1, chips):
            later_hop(k, hop)
        if chips > 1:
            forward(2 * hop - 4)
            forward(2 * hop - 3)
        return carry

    lax.fori_loop(2, hops, hop_step, 0)
    for k in range(1, chips):
        later_hop(k, jnp.int32(hops))
    if chips > 1:
        forward(n - 4)
        forward(n - 3)
    for k in range(chips):
        close_part(k)
    if chips > 1:
        forward(n - 2)
        forward(n - 1)

    for side in range(2):
        for k in range(chips):
            ring_hop(k, side, hops - 1, whole if hops > 2 else halves[side]).wait_send()
            ring_hop(k, side, hops, whole).wait_send()

        def low_out(hop, carry, side=side):
            for u in range(hops):

                @pl.when((u < hop) & carried(side, hop, u, None, 0))
                def _(u=u):
                    low_hop(side, hop, u).wait_send()

            return carry

        lax.fori_loop(1, hops + 1, low_out, 0)
    for k in range(chips):
        gram_send(k).wait_send()
    for k in range(1, chips):
        gram_forward(k).wait_send()
    for k in range(1, parts):
        remote(d_ring, dt_ref.at[col], dc_send.at[k], dc_recv.at[k], {"col": (col + k) % parts}).wait()

    def shared(t, carry):
        for k in range(chips):
            item_send(k, t).wait_send()
        item_send(0, t).wait_recv()
        for k in range(1, chips):
            item_forward(k, t).wait()
        return carry

    lax.fori_loop(0, n, shared, 0)


def reduce_columns(n, parts, gt, flat, slab, diag):
    slab_cols, depth = gt.shape
    rows = slab.shape[0]
    q = flat.shape[1] // n
    tile = depth // 7 if depth % 112 == 0 else depth
    hops, chips, span = n // 2, parts // 2, 2 * slab_cols
    slots = hops * (hops + 1) // 2
    f32, bf16 = jnp.float32, jnp.bfloat16
    vmem, any_space = pl.BlockSpec(memory_space=pltpu.VMEM), pl.BlockSpec(memory_space=pl.ANY)
    dma = pltpu.SemaphoreType.DMA
    both = lambda *shape: [dma(shape), dma(shape)]
    return pl.pallas_call(
        functools.partial(reduce_kernel, n, parts),
        out_shape=(
            jax.ShapeDtypeStruct((n * rows, q), f32),
            jax.ShapeDtypeStruct((parts, n, rows, slab_cols), bf16),
            jax.ShapeDtypeStruct((parts, n) + diag.shape, f32),
        ),
        in_specs=[any_space, any_space, vmem, vmem],
        out_specs=(vmem, any_space, vmem),
        scratch_shapes=[
            pltpu.VMEM((n, depth, q), bf16),
            pltpu.VMEM((2, tile, n * q), bf16),
            pltpu.VMEM((parts * slab_cols, depth), bf16),
            pltpu.VMEM((2, 2, chips, span, q), bf16),
            pltpu.VMEM((2, 2, chips, span, q), bf16),
            pltpu.VMEM((2, span, q), f32),
            pltpu.VMEM((rows, depth), bf16),
            pltpu.VMEM((2, slots, rows, q), bf16),
            pltpu.VMEM((2, slots, rows, q), bf16),
            pltpu.VMEM((n,) + diag.shape, f32),
            dma((2,)),
            dma,
            *both(2 * chips),
            *both(chips, 2, hops),
            dma,
            *both(2, hops),
            *both(2, hops),
            *both(chips, n),
            *both(max(chips - 1, 1), n),
            *both(parts),
            *both(2, slots),
        ],
        compiler_params=pltpu.CompilerParams(collective_id=1, has_side_effects=True, vmem_limit_bytes=VMEM_BYTES),
    )(gt, flat, slab, diag)


def solve_kernel(
    n, parts, direction, t_ref, dt_ref, om_ref, or_ref,
    tv, d_ref, v, residual, mapped, out_m, out_r, t_sem, send, recv,
):
    me = lax.axis_index("row")
    rows, q = om_ref.shape[1], om_ref.shape[2]
    depth = tv.shape[3]
    f32 = jnp.float32

    barrier = pltpu.get_barrier_semaphore()
    for k in range(1, n):
        pl.semaphore_signal(barrier, inc=1, device_id={"row": (me + k) % n}, device_id_type=MESH)

    def load(i):
        return pltpu.make_async_copy(t_ref.at[:, i], tv.at[i], t_sem.at[i])

    for i in range(n):
        load(i).start()

    def block(i):
        return pl.ds(pl.multiple_of(i * rows, 16), rows)

    for i in range(n):
        lines = dt_ref[0, i]
        for c in range(1, parts):
            lines += dt_ref[c, i]
        for line in range(pl.cdiv(rows, 128)):
            size = min(128, rows - line * 128)
            square = jnp.broadcast_to(lines[line : line + 1, :], (size, 128))
            lanes = lax.broadcasted_iota(jnp.int32, square.shape, 1)
            chosen = lanes == lax.broadcasted_iota(jnp.int32, square.shape, 0)
            value = jnp.sum(jnp.where(chosen, square, 0.0), axis=1, keepdims=True)
            d_ref[pl.ds(i * rows + line * 128, size), :] = value

    def product(loading, toward):
        def step(i, carry):
            if loading:
                load(i).wait()
            here = block(i)
            total = jnp.zeros((rows, q), f32)
            for c in range(parts):
                total += jnp.dot(tv[i, c], v[pl.ds(c * depth, depth), :], preferred_element_type=f32)
            result = 0.9 * total + d_ref[here, :] * v[here, :].astype(f32)
            mapped[here, :] = result
            return carry + jnp.sum(toward(here) * result, axis=0, keepdims=True)

        return lax.fori_loop(0, n, step, jnp.zeros((1, q), f32))

    def column_sum(terms):
        def step(i, total):
            return total + jnp.sum(terms(block(i)), axis=0, keepdims=True)

        return lax.fori_loop(0, n, step, jnp.zeros((1, q), f32))

    def first(here):
        start = direction[here, :]
        v[here, :] = start.astype(jnp.bfloat16)
        return start * start

    norm = column_sum(first)
    curvature = product(True, lambda here: direction[here, :])
    step_a = norm / curvature

    def second(here):
        left = direction[here, :] - step_a * mapped[here, :]
        residual[here, :] = left
        return left * left

    norm_next = column_sum(second)
    scale = norm_next / norm

    def turn(i, carry):
        here = block(i)
        v[here, :] = (residual[here, :] + scale * direction[here, :]).astype(jnp.bfloat16)
        return carry

    lax.fori_loop(0, n, turn, 0)
    curvature = product(False, lambda here: residual[here, :] + scale * direction[here, :])
    step_b = norm_next / curvature

    pl.semaphore_wait(barrier, n - 1)

    def leaving(k):
        i = (me + k) % n
        return [
            remote(held.at[block(i), :], target.at[me], send.at[kind, k], recv.at[kind, k], {"row": i})
            for kind, held, target in ((0, out_m, om_ref), (1, out_r, or_ref))
        ]

    def outputs(i):
        here = block(i)
        left, start = residual[here, :], direction[here, :]
        merged = step_a * start + step_b * (left + scale * start)
        return merged.astype(jnp.bfloat16), (left - step_b * mapped[here, :]).astype(jnp.bfloat16)

    def finish(k, carry):
        i = (me + k) % n
        here = block(i)
        out_m[here, :], out_r[here, :] = outputs(i)

        @pl.when(k > 1)
        def _():
            for copy in leaving(k - 1):
                copy.start()

        return carry

    lax.fori_loop(1, n, finish, 0)
    om_ref[me], or_ref[me] = outputs(me)
    for copy in leaving(n - 1):
        copy.start()

    def drain(k, carry):
        for copy in leaving(k):
            copy.wait()
        return carry

    lax.fori_loop(1, n, drain, 0)


def solve(n, start, total, diag):
    parts = total.shape[0]
    all_rows, q = start.shape
    vmem = pl.BlockSpec(memory_space=pltpu.VMEM)
    half, full = pltpu.VMEM((all_rows, q), jnp.bfloat16), pltpu.VMEM((all_rows, q), jnp.float32)
    out = jax.ShapeDtypeStruct((n, all_rows // n, q), jnp.bfloat16)
    return pl.pallas_call(
        functools.partial(solve_kernel, n, parts),
        out_shape=(out, out),
        in_specs=[vmem, pl.BlockSpec(memory_space=pl.ANY), vmem],
        out_specs=(vmem, vmem),
        scratch_shapes=[
            pltpu.VMEM((n, parts) + total.shape[2:], jnp.bfloat16),
            pltpu.VMEM((all_rows, 1), jnp.float32),
            half,
            full,
            full,
            half,
            half,
            pltpu.SemaphoreType.DMA((n,)),
            pltpu.SemaphoreType.DMA((2, n)),
            pltpu.SemaphoreType.DMA((2, n)),
        ],
        compiler_params=pltpu.CompilerParams(collective_id=2, has_side_effects=True, vmem_limit_bytes=VMEM_BYTES),
    )(start, total, diag)


def join_kernel(a_ref, b_ref, a_out, b_out):
    n, _, q = a_ref.shape
    for source, target in ((a_ref, a_out), (b_ref, b_out)):
        for j in range(n):
            target[:, j * q : (j + 1) * q] = source[j].astype(target.dtype)


def join_columns(a, b):
    n, rows, q = a.shape
    tile = rows // 7 if rows % 112 == 0 else rows
    out = jax.ShapeDtypeStruct((rows, n * q), jnp.float32)
    taken = pl.BlockSpec((n, tile, q), lambda i: (0, i, 0))
    given = pl.BlockSpec((tile, n * q), lambda i: (i, 0))
    return pl.pallas_call(
        join_kernel, grid=(rows // tile,), out_shape=(out, out), in_specs=[taken, taken], out_specs=(given, given)
    )(a, b)


def shards(n, parts, grams, weights):
    models, rows, slab_cols = grams.shape

    own_total = jnp.sum(grams.astype(jnp.float32), axis=0)
    row_ids = lax.axis_index("row") * rows + jnp.arange(rows)[:, None]
    col_ids = lax.axis_index("col") * slab_cols + jnp.arange(slab_cols)[None, :]
    diagonal = row_ids == col_ids
    slab = jnp.where(diagonal, 0.0, own_total).astype(jnp.bfloat16)
    own_diag = jnp.sum(jnp.where(diagonal, own_total, 0.0), axis=1)
    padded = -(-rows // 1024) * 1024
    own_diag = jnp.pad(own_diag, (0, padded - rows)).reshape(-1, 128)

    transposed = grams.transpose(2, 0, 1).reshape(slab_cols, models * rows)
    flat = weights.reshape(models * rows, -1)
    start, total, diags = reduce_columns(n, parts, transposed, flat, slab, own_diag)
    merged, residual = solve(n, start, total, diags)
    return join_columns(merged, residual)


def solution(mesh):
    placed = (P(None, "row", "col"), P(None, "row", "col"))
    return jax.shard_map(
        functools.partial(shards, mesh.shape["row"], mesh.shape["col"]),
        mesh=mesh,
        in_specs=placed,
        out_specs=(P("row", "col"), P("row", "col")),
        check_vma=False,
    )
```

```python
import functools

import jax
import jax.numpy as jnp
from jax import lax
from jax.experimental import pallas as pl
from jax.experimental.pallas import tpu as pltpu
from jax.sharding import PartitionSpec as P

ITERS = 2
MESH = pl.DeviceIdType.MESH
VMEM_BYTES = 63 * 2**20


def ring_position(index, n):
    odd = index % 2
    return (1 - odd) * (index // 2) + odd * (n - 1 - index // 2)


def ring_index(position, n):
    back = position // (n // 2)
    return (1 - back) * 2 * position + back * (2 * (n - 1 - position) + 1)


def remote(source, target, send, recv, where):
    return pltpu.make_async_remote_copy(
        src_ref=source, dst_ref=target, send_sem=send, recv_sem=recv, device_id=where, device_id_type=MESH
    )


def reduce_kernel(
    n, parts, gt_ref, flat_ref, slab_ref, d_ref, out_ref, t_ref, dt_ref,
    w_ref, staged, gt, sent, came, part, e_block, lo_sent, lo_came, d_ring,
    w_sem, g_own, g_send, g_recv, r_send, r_recv, t_own, t_send, t_recv, td_send, td_recv,
    x_send, x_recv, f_send, f_recv, dc_send, dc_recv, lo_send, lo_recv,
):
    f32, bf16 = jnp.float32, jnp.bfloat16
    row, col = lax.axis_index("row"), lax.axis_index("col")
    place = ring_position(row, n)
    chips, hops = parts // 2, n // 2
    chip, core = col // 2, col % 2
    rows, slab_cols = slab_ref.shape
    q = out_ref.shape[1]
    span = 2 * slab_cols
    half = span // 2
    cut = rows // 32 * 16
    twin = {"col": chip * 2 + 1 - core}

    def at(distance):
        return ring_index((place + n + distance) % n, n)

    right, left = {"row": at(1)}, {"row": at(-1)}

    def peer(k):
        return {"col": (chip + k) % chips * 2 + core}

    def cols_of(c):
        return pl.ds(pl.multiple_of(c * slab_cols, 16), slab_cols)

    def block(i):
        return pl.ds(pl.multiple_of(i * rows, 16), rows)

    barrier = pltpu.get_barrier_semaphore()
    for k in range(1, n):
        pl.semaphore_signal(barrier, inc=1, device_id={"row": (row + k) % n}, device_id_type=MESH)
    for k in range(1, parts):
        pl.semaphore_signal(barrier, inc=1, device_id={"col": (col + k) % parts}, device_id_type=MESH)
    own_gt = pltpu.make_async_copy(gt_ref, gt.at[cols_of(col), :], g_own)
    own_gt.start()
    own_slab = pltpu.make_async_copy(slab_ref, t_ref.at[col, row], t_own)
    own_slab.start()
    d_ring[row] = d_ref[...]
    zeros = jnp.zeros((half, q), bf16)
    for k in range(chips):
        came[0, 0, k, half:, :] = zeros
        came[1, 0, k, :half, :] = zeros
    pl.semaphore_wait(barrier, n - 1 + parts - 1)

    def gram_send(k):
        return remote(gt_ref, gt.at[cols_of(col), :], g_send.at[k], g_recv.at[k], peer(k) if k else twin)

    def gram_forward(k):
        origin = gt.at[cols_of((chip + chips - k) % chips * 2 + core), :]
        return remote(origin, origin, g_send.at[chips + k - 1], g_recv.at[chips + k - 1], twin)

    for k in range(chips):
        gram_send(k).start()

    def slab_hop(side, hop, kind):
        owner = at(1 - hop) if side == 0 else at(hop - 1)
        held = t_ref.at[col, owner]
        if kind == "half":
            held = t_ref.at[col, owner, pl.ds(0, cut), :] if side == 0 else t_ref.at[col, owner, pl.ds(cut, rows - cut), :]
        source = slab_ref if kind == "own" else held
        to = left if side else right
        return remote(source, held, t_send.at[side, hop - 1], t_recv.at[side, hop - 1], to)

    def diag_hop(side, hop):
        held = d_ring.at[at(1 - hop) if side == 0 else at(hop - 1)]
        return remote(held, held, td_send.at[side, hop - 1], td_recv.at[side, hop - 1], left if side else right)

    def slab_start(hop, kind):
        for side in range(2):
            slab_hop(side, hop, kind).start()
            if kind != "half" or side == 0:
                diag_hop(side, hop).start()

    def slab_wait(hop, kind):
        for side in range(2):
            slab_hop(side, hop, kind).wait()
            if kind != "half" or side == 0:
                diag_hop(side, hop).wait()

    def item(t):
        return t_ref.at[col, at((1 - 2 * (t % 2)) * ((t + 1) // 2))]

    def item_send(k, t):
        return remote(item(t), item(t), x_send.at[k, t], x_recv.at[k, t], peer(k) if k else twin)

    def item_forward(k, t):
        origin = (chip + chips - k) % chips * 2 + core
        held = t_ref.at[origin, at((1 - 2 * (t % 2)) * ((t + 1) // 2))]
        return remote(held, held, f_send.at[k - 1, t], f_recv.at[k - 1, t], twin)

    def share(t):
        for k in list(range(1, chips)) + [0]:
            item_send(k, t).start()

    def forward(t):
        for k in range(1, chips):
            item_send(k, t).wait_recv()
            item_forward(k, t).start()

    def partial(side, target, base):
        def step(i, carry):
            here = pl.ds(pl.multiple_of(base + i * rows, 16), rows)
            part[side, block(i), :] = jnp.dot(gt[here, :], w_ref[target], preferred_element_type=f32)
            return carry

        lax.fori_loop(0, span // rows, step, 0)

    def ring_hop(k, side, hop, window):
        slot_of = (hop - 1) % 2
        return remote(
            sent.at[side, slot_of, k, window, :],
            came.at[side, slot_of, k, window, :],
            r_send.at[k, side, hop - 1],
            r_recv.at[k, side, hop - 1],
            left if side else right,
        )

    halves = (pl.ds(0, half), pl.ds(half, span - half))
    whole = pl.ds(0, span)

    def slot(hop, u):
        return hop * (hop - 1) // 2 + u

    def low_hop(side, hop, u):
        here = slot(hop, u)
        return remote(
            lo_sent.at[side, here],
            lo_came.at[side, here],
            lo_send.at[side, here],
            lo_recv.at[side, here],
            left if side else right,
        )

    def member(side, u):
        return at((2 * side - 1) * u)

    def carried(side, hop, u, source, shift):
        first = member(side, u + shift) * rows
        used = (u < hop - 1) | ((first % span) // half == side)
        return used if source is None else used & (first // span == source)

    def diag_term(target):
        return jnp.dot(e_block[...], w_ref[target], preferred_element_type=f32) * (1 / 9)

    def source_of(k):
        return (chip + k) % chips

    def extract(k):
        @pl.when(row * rows // span == source_of(k))
        def _():
            mine = gt[block(row), :]
            lanes = lax.broadcasted_iota(jnp.int32, mine.shape, 1)
            below = lanes - lax.broadcasted_iota(jnp.int32, mine.shape, 0)
            chosen = below == 0
            for model in range(1, mine.shape[1] // rows):
                chosen = chosen | (below == model * rows)
            e_block[...] = jnp.where(chosen, mine.astype(f32), 0.0).astype(bf16)

    def split(k, side, hop, u, value):
        here = pl.ds(pl.multiple_of(member(side, u) * rows - source_of(k) * span, 16), rows)
        high = value.astype(bf16)
        sent[side, (hop - 1) % 2, k, here, :] = high
        lo_sent[side, slot(hop, u)] = (value - high.astype(f32)).astype(bf16)

    def local(k, side, u):
        return pl.ds(pl.multiple_of(member(side, u) * rows - source_of(k) * span, 16), rows)

    def first_hop(k):
        extract(k)
        partial(0, at(hops), source_of(k) * span)
        for side in range(2):
            sent[side, 0, k, halves[side], :] = part[0, halves[side], :].astype(bf16)

            @pl.when(carried(side, 1, 0, source_of(k), 0))
            def _(side=side):
                split(k, side, 1, 0, part[0, local(k, side, 0), :] + diag_term(at(hops)))

        for side in range(2):
            ring_hop(k, side, 1, halves[side]).start()

            @pl.when(carried(side, 1, 0, source_of(k), 0))
            def _(side=side):
                low_hop(side, 1, 0).start()

    def later_hop(k, hop):
        source = source_of(k)

        def side_partial(side, carry):
            partial(side, at((1 - 2 * side) * (hops + 1 - hop)), source * span)
            return carry

        lax.fori_loop(0, 2, side_partial, 0)
        for side in range(2):

            @pl.when(hop == 2)
            def _(side=side):
                ring_hop(k, side, 1, halves[side]).wait_recv()

            @pl.when(hop > 2)
            def _(side=side):
                ring_hop(k, side, hop - 1, whole).wait_recv()

            @pl.when(hop == 3)
            def _(side=side):
                ring_hop(k, side, 1, halves[side]).wait_send()

            @pl.when(hop > 3)
            def _(side=side):
                ring_hop(k, side, hop - 2, whole).wait_send()

            def add(i, carry, side=side):
                value = part[side, block(i), :] + came[side, hop % 2, k, block(i), :].astype(f32)
                sent[side, (hop - 1) % 2, k, block(i), :] = value.astype(bf16)
                return carry

            lax.fori_loop(0, span // rows, add, 0)
            for u in range(hops):

                @pl.when((u < hop) & carried(side, hop, u, source, 0))
                def _(side=side, u=u):
                    here = local(k, side, u)
                    value = part[side, here, :] + came[side, hop % 2, k, here, :].astype(f32)
                    if u == 0:
                        value += diag_term(at((1 - 2 * side) * (hops + 1 - hop)))
                    else:
                        low_hop(side, hop - 1, u - 1).wait_recv()
                        value += lo_came[side, slot(hop - 1, u - 1)].astype(f32)
                    split(k, side, hop, u, value)

        for side in range(2):
            ring_hop(k, side, hop, whole).start()
            for u in range(hops):

                @pl.when((u < hop) & carried(side, hop, u, source, 0))
                def _(side=side, u=u):
                    low_hop(side, hop, u).start()

    def close_part(k):
        source = source_of(k)
        partial(0, row, source * span)
        for side in range(2):
            ring_hop(k, side, hops, whole).wait_recv()

        def close(i, carry):
            value = part[0, block(i), :]
            for side in range(2):
                value += came[side, (hops - 1) % 2, k, block(i), :].astype(f32)
            out_ref[pl.ds(pl.multiple_of(source * span + i * rows, 16), rows), :] = 0.9 * value
            return carry

        lax.fori_loop(0, span // rows, close, 0)

        @pl.when(row * rows // span == source)
        def _():
            out_ref[block(row), :] += 0.9 * diag_term(row)

        for side in range(2):
            for u in range(hops):

                @pl.when(carried(side, hops, u, source, 1))
                def _(side=side, u=u):
                    low_hop(side, hops, u).wait_recv()
                    out_ref[block(member(side, u + 1)), :] += 0.9 * lo_came[side, slot(hops, u)].astype(f32)

    tile = staged.shape[1]
    tiles = w_ref.shape[1] // tile

    def staging(i):
        source = flat_ref.at[pl.ds(pl.multiple_of(i * tile, 16), tile), :]
        return pltpu.make_async_copy(source, staged.at[i % 2], w_sem.at[i % 2])

    def spread(i, carry):
        @pl.when(i + 1 < tiles)
        def _():
            staging(i + 1).start()

        staging(i).wait()
        for j in range(n):
            w_ref[j, pl.ds(pl.multiple_of(i * tile, 16), tile), :] = staged[i % 2, :, j * q : (j + 1) * q]
        return carry

    slab_start(1, "own")
    staging(0).start()
    own_slab.wait()
    share(0)
    lax.fori_loop(0, tiles, spread, 0)
    own_gt.wait()
    gram_send(0).wait_recv()
    first_hop(0)

    def slab_step(hop, carry):
        slab_wait(hop - 1, "full")
        slab_start(hop, "full")
        share(2 * (hop - 1) - 1)
        share(2 * (hop - 1))
        return carry

    lax.fori_loop(2, hops, slab_step, 0)
    slab_wait(hops - 1, "full")
    slab_start(hops, "half")
    share(n - 3)
    share(n - 2)
    for k in range(1, chips):
        gram_send(k).wait_recv()
        gram_forward(k).start()
    for k in range(1, chips):
        gram_forward(k).wait_recv()
        first_hop(k)
    slab_wait(hops, "half")
    share(n - 1)
    dt_ref[col] = d_ring[...]
    for k in range(1, parts):
        remote(d_ring, dt_ref.at[col], dc_send.at[k], dc_recv.at[k], {"col": (col + k) % parts}).start()

    def hop_step(hop, carry):
        for k in range(chips):
            later_hop(k, hop)
        if chips > 1:
            forward(2 * hop - 4)
            forward(2 * hop - 3)
        return carry

    lax.fori_loop(2, hops + 1, hop_step, 0)
    for k in range(chips):
        close_part(k)
    if chips > 1:
        forward(n - 2)
        forward(n - 1)

    for side in range(2):
        for k in range(chips):
            ring_hop(k, side, hops - 1, whole if hops > 2 else halves[side]).wait_send()
            ring_hop(k, side, hops, whole).wait_send()

        def low_out(hop, carry, side=side):
            for u in range(hops):

                @pl.when((u < hop) & carried(side, hop, u, None, 0))
                def _(u=u):
                    low_hop(side, hop, u).wait_send()

            return carry

        lax.fori_loop(1, hops + 1, low_out, 0)
    for k in range(chips):
        gram_send(k).wait_send()
    for k in range(1, chips):
        gram_forward(k).wait_send()
    for k in range(1, parts):
        remote(d_ring, dt_ref.at[col], dc_send.at[k], dc_recv.at[k], {"col": (col + k) % parts}).wait()

    def shared(t, carry):
        for k in range(chips):
            item_send(k, t).wait_send()
        item_send(0, t).wait_recv()
        for k in range(1, chips):
            item_forward(k, t).wait()
        return carry

    lax.fori_loop(0, n, shared, 0)


def reduce_columns(n, parts, gt, flat, slab, diag):
    slab_cols, depth = gt.shape
    rows = slab.shape[0]
    q = flat.shape[1] // n
    tile = depth // 7 if depth % 112 == 0 else depth
    hops, chips, span = n // 2, parts // 2, 2 * slab_cols
    slots = hops * (hops + 1) // 2
    f32, bf16 = jnp.float32, jnp.bfloat16
    vmem, any_space = pl.BlockSpec(memory_space=pltpu.VMEM), pl.BlockSpec(memory_space=pl.ANY)
    dma = pltpu.SemaphoreType.DMA
    both = lambda *shape: [dma(shape), dma(shape)]
    return pl.pallas_call(
        functools.partial(reduce_kernel, n, parts),
        out_shape=(
            jax.ShapeDtypeStruct((n * rows, q), f32),
            jax.ShapeDtypeStruct((parts, n, rows, slab_cols), bf16),
            jax.ShapeDtypeStruct((parts, n) + diag.shape, f32),
        ),
        in_specs=[any_space, any_space, vmem, vmem],
        out_specs=(vmem, any_space, vmem),
        scratch_shapes=[
            pltpu.VMEM((n, depth, q), bf16),
            pltpu.VMEM((2, tile, n * q), bf16),
            pltpu.VMEM((parts * slab_cols, depth), bf16),
            pltpu.VMEM((2, 2, chips, span, q), bf16),
            pltpu.VMEM((2, 2, chips, span, q), bf16),
            pltpu.VMEM((2, span, q), f32),
            pltpu.VMEM((rows, depth), bf16),
            pltpu.VMEM((2, slots, rows, q), bf16),
            pltpu.VMEM((2, slots, rows, q), bf16),
            pltpu.VMEM((n,) + diag.shape, f32),
            dma((2,)),
            dma,
            *both(2 * chips),
            *both(chips, 2, hops),
            dma,
            *both(2, hops),
            *both(2, hops),
            *both(chips, n),
            *both(max(chips - 1, 1), n),
            *both(parts),
            *both(2, slots),
        ],
        compiler_params=pltpu.CompilerParams(collective_id=1, has_side_effects=True, vmem_limit_bytes=VMEM_BYTES),
    )(gt, flat, slab, diag)


def solve_kernel(
    n, parts, direction, t_ref, dt_ref, om_ref, or_ref,
    tv, d_ref, v, residual, mapped, out_m, out_r, t_sem, send, recv,
):
    me = lax.axis_index("row")
    rows, q = om_ref.shape[1], om_ref.shape[2]
    depth = tv.shape[3]
    f32 = jnp.float32

    barrier = pltpu.get_barrier_semaphore()
    for k in range(1, n):
        pl.semaphore_signal(barrier, inc=1, device_id={"row": (me + k) % n}, device_id_type=MESH)

    def load(i):
        return pltpu.make_async_copy(t_ref.at[:, i], tv.at[i], t_sem.at[i])

    for i in range(n):
        load(i).start()

    def block(i):
        return pl.ds(pl.multiple_of(i * rows, 16), rows)

    for i in range(n):
        lines = dt_ref[0, i]
        for c in range(1, parts):
            lines += dt_ref[c, i]
        for line in range(pl.cdiv(rows, 128)):
            size = min(128, rows - line * 128)
            square = jnp.broadcast_to(lines[line : line + 1, :], (size, 128))
            lanes = lax.broadcasted_iota(jnp.int32, square.shape, 1)
            chosen = lanes == lax.broadcasted_iota(jnp.int32, square.shape, 0)
            value = jnp.sum(jnp.where(chosen, square, 0.0), axis=1, keepdims=True)
            d_ref[pl.ds(i * rows + line * 128, size), :] = value

    def product(loading, toward):
        def step(i, carry):
            if loading:
                load(i).wait()
            here = block(i)
            total = jnp.zeros((rows, q), f32)
            for c in range(parts):
                total += jnp.dot(tv[i, c], v[pl.ds(c * depth, depth), :], preferred_element_type=f32)
            result = 0.9 * total + d_ref[here, :] * v[here, :].astype(f32)
            mapped[here, :] = result
            return carry + jnp.sum(toward(here) * result, axis=0, keepdims=True)

        return lax.fori_loop(0, n, step, jnp.zeros((1, q), f32))

    def column_sum(terms):
        def step(i, total):
            return total + jnp.sum(terms(block(i)), axis=0, keepdims=True)

        return lax.fori_loop(0, n, step, jnp.zeros((1, q), f32))

    def first(here):
        start = direction[here, :]
        v[here, :] = start.astype(jnp.bfloat16)
        return start * start

    norm = column_sum(first)
    curvature = product(True, lambda here: direction[here, :])
    step_a = norm / curvature

    def second(here):
        left = direction[here, :] - step_a * mapped[here, :]
        residual[here, :] = left
        return left * left

    norm_next = column_sum(second)
    scale = norm_next / norm

    def turn(i, carry):
        here = block(i)
        v[here, :] = (residual[here, :] + scale * direction[here, :]).astype(jnp.bfloat16)
        return carry

    lax.fori_loop(0, n, turn, 0)
    curvature = product(False, lambda here: residual[here, :] + scale * direction[here, :])
    step_b = norm_next / curvature

    pl.semaphore_wait(barrier, n - 1)

    def leaving(k):
        i = (me + k) % n
        return [
            remote(held.at[block(i), :], target.at[me], send.at[kind, k], recv.at[kind, k], {"row": i})
            for kind, held, target in ((0, out_m, om_ref), (1, out_r, or_ref))
        ]

    def outputs(i):
        here = block(i)
        left, start = residual[here, :], direction[here, :]
        merged = step_a * start + step_b * (left + scale * start)
        return merged.astype(jnp.bfloat16), (left - step_b * mapped[here, :]).astype(jnp.bfloat16)

    def finish(k, carry):
        i = (me + k) % n
        here = block(i)
        out_m[here, :], out_r[here, :] = outputs(i)

        @pl.when(k > 1)
        def _():
            for copy in leaving(k - 1):
                copy.start()

        return carry

    lax.fori_loop(1, n, finish, 0)
    om_ref[me], or_ref[me] = outputs(me)
    for copy in leaving(n - 1):
        copy.start()

    def drain(k, carry):
        for copy in leaving(k):
            copy.wait()
        return carry

    lax.fori_loop(1, n, drain, 0)


def solve(n, start, total, diag):
    parts = total.shape[0]
    all_rows, q = start.shape
    vmem = pl.BlockSpec(memory_space=pltpu.VMEM)
    half, full = pltpu.VMEM((all_rows, q), jnp.bfloat16), pltpu.VMEM((all_rows, q), jnp.float32)
    out = jax.ShapeDtypeStruct((n, all_rows // n, q), jnp.bfloat16)
    return pl.pallas_call(
        functools.partial(solve_kernel, n, parts),
        out_shape=(out, out),
        in_specs=[vmem, pl.BlockSpec(memory_space=pl.ANY), vmem],
        out_specs=(vmem, vmem),
        scratch_shapes=[
            pltpu.VMEM((n, parts) + total.shape[2:], jnp.bfloat16),
            pltpu.VMEM((all_rows, 1), jnp.float32),
            half,
            full,
            full,
            half,
            half,
            pltpu.SemaphoreType.DMA((n,)),
            pltpu.SemaphoreType.DMA((2, n)),
            pltpu.SemaphoreType.DMA((2, n)),
        ],
        compiler_params=pltpu.CompilerParams(collective_id=2, has_side_effects=True, vmem_limit_bytes=VMEM_BYTES),
    )(start, total, diag)


def join_kernel(a_ref, b_ref, a_out, b_out):
    n, _, q = a_ref.shape
    for source, target in ((a_ref, a_out), (b_ref, b_out)):
        for j in range(n):
            target[:, j * q : (j + 1) * q] = source[j].astype(target.dtype)


def join_columns(a, b):
    n, rows, q = a.shape
    tile = rows // 7 if rows % 112 == 0 else rows
    out = jax.ShapeDtypeStruct((rows, n * q), jnp.float32)
    taken = pl.BlockSpec((n, tile, q), lambda i: (0, i, 0))
    given = pl.BlockSpec((tile, n * q), lambda i: (i, 0))
    return pl.pallas_call(
        join_kernel, grid=(rows // tile,), out_shape=(out, out), in_specs=[taken, taken], out_specs=(given, given)
    )(a, b)


def shards(n, parts, grams, weights):
    models, rows, slab_cols = grams.shape

    own_total = jnp.sum(grams.astype(jnp.float32), axis=0)
    row_ids = lax.axis_index("row") * rows + jnp.arange(rows)[:, None]
    col_ids = lax.axis_index("col") * slab_cols + jnp.arange(slab_cols)[None, :]
    diagonal = row_ids == col_ids
    slab = jnp.where(diagonal, 0.0, own_total).astype(jnp.bfloat16)
    own_diag = jnp.sum(jnp.where(diagonal, own_total, 0.0), axis=1)
    padded = -(-rows // 1024) * 1024
    own_diag = jnp.pad(own_diag, (0, padded - rows)).reshape(-1, 128)

    transposed = grams.transpose(2, 0, 1).reshape(slab_cols, models * rows)
    flat = weights.reshape(models * rows, -1)
    start, total, diags = reduce_columns(n, parts, transposed, flat, slab, own_diag)
    merged, residual = solve(n, start, total, diags)
    return join_columns(merged, residual)


def solution(mesh):
    placed = (P(None, "row", "col"), P(None, "row", "col"))
    return jax.shard_map(
        functools.partial(shards, mesh.shape["row"], mesh.shape["col"]),
        mesh=mesh,
        in_specs=placed,
        out_specs=(P("row", "col"), P("row", "col")),
        check_vma=False,
    )
```
